64 devices in a mesh: data: 4 (over x, y), model: 16 (over z, core).
Axes of the slice: x: 2, y: 2, z: 8, core: 2. Of those that a mesh axis runs over, the one named last changes fastest.
The devices are a block of a 4x4x8 slice.
Arguments:
- resid_x: bfloat16 [16384, 2048], P('data'), parts along dimension 0
- ln_mean: float32 [16384], P('data'), parts along dimension 0
- ln_rstd: float32 [16384], P('data'), parts along dimension 0
- ln_gain: bfloat16 [2048], replicated
- grad_y: bfloat16 [16384, 2048], P('data'), parts along dimension 0
- w_qkv: bfloat16 [2048, 6144], P(None, 'model')
- w_out: bfloat16 [16, 128, 2048], P('model')
- w_up: bfloat16 [2048, 8192], P(None, 'model')
- w_down: bfloat16 [8192, 2048], P('model')
Outputs:
- output 1: bfloat16 [16384, 2048], P('data'), parts along dimension 0
- output 2: bfloat16 [8192, 6144], P('data', 'model'), parts along dimension 0
- output 3: bfloat16 [64, 128, 2048], P(('data', 'model')), parts along dimension 0
- output 4: bfloat16 [8192, 8192], P('data', 'model'), parts along dimension 0
- output 5: bfloat16 [32768, 2048], P(('data', 'model')), parts along dimension 0
There are 4 independent parts. The reference program is written for one: setup_inputs(seed, part) draws one part's arguments, and reference() takes and returns one part's arrays. A program takes and returns all parts, laid end to end along the dimension named above; an argument that names none is the same for every part.
All inputs are finite; a program needn't handle non-finite values.
Results may differ from the reference program's by a relative error of at most 0.0168419.
Values are sent between devices in bfloat16 or wider.
A program may use at most 768 MiB of HBM per device.

```python
import jax
import jax.numpy as jnp
from jax import lax

TOKENS = 4096
D = 2048
HEADS = 16
FF = 8192

HEAD = D // HEADS
ROT = HEAD // 4
HALF = ROT // 2


def setup_inputs(seed: int = 0, part: int = 0) -> dict:
    part_key = jax.random.fold_in(jax.random.key(seed), part)
    key_x, key_rows, key_off, key_dy = jax.random.split(part_key, 4)
    key_gain, key_qkv, key_out, key_up, key_down = jax.random.split(jax.random.key(seed + 1), 5)
    row_scale = 0.8 * jnp.exp2(jax.random.uniform(key_rows, (TOKENS, 1), jnp.float32, -1.0, 1.0))
    row_offset = 0.5 * jax.random.normal(key_off, (TOKENS, 1), jnp.float32)
    resid_x = (row_scale * jax.random.normal(key_x, (TOKENS, D), jnp.float32) + row_offset).astype(jnp.bfloat16)
    x_f32 = resid_x.astype(jnp.float32)
    ln_mean = jnp.mean(x_f32, axis=1)
    ln_rstd = lax.rsqrt(jnp.mean(jnp.square(x_f32 - ln_mean[:, None]), axis=1) + 1e-5)
    ln_gain = (1.0 + 0.3 * jax.random.normal(key_gain, (D,), jnp.float32)).astype(jnp.bfloat16)
    grad_y = jax.random.normal(key_dy, (TOKENS, D), jnp.float32).astype(jnp.bfloat16)
    fan_d = D ** -0.5
    w_qkv = (1.5 * fan_d * jax.random.normal(key_qkv, (D, 3 * D), jnp.float32)).astype(jnp.bfloat16)
    w_out = (2.0 * fan_d * jax.random.normal(key_out, (HEADS, HEAD, D), jnp.float32)).astype(jnp.bfloat16)
    w_up = (fan_d * jax.random.normal(key_up, (D, FF), jnp.float32)).astype(jnp.bfloat16)
    w_down = (FF ** -0.5 * jax.random.normal(key_down, (FF, D), jnp.float32)).astype(jnp.bfloat16)
    return {"resid_x": resid_x, "ln_mean": ln_mean, "ln_rstd": ln_rstd, "ln_gain": ln_gain, "grad_y": grad_y, "w_qkv": w_qkv, "w_out": w_out, "w_up": w_up, "w_down": w_down}


def rope_tables():
    positions = jnp.arange(TOKENS, dtype=jnp.float32)[:, None]
    inv_freq = jnp.power(10000.0, -2.0 * jnp.arange(HALF, dtype=jnp.float32) / ROT)
    angles = positions * inv_freq[None, :]
    return jnp.cos(angles)[:, None, :], jnp.sin(angles)[:, None, :]


def rotate(vectors, rope_cos, rope_sin):
    first_half = vectors[..., :HALF]
    second_half = vectors[..., HALF:ROT]
    return jnp.concatenate([first_half * rope_cos - second_half * rope_sin, second_half * rope_cos + first_half * rope_sin, vectors[..., ROT:]], axis=-1)


def exact_gelu(pre_act):
    return jax.nn.gelu(pre_act, approximate=False)


def head_pass(operands):
    q_head, k_head, v_head, d_head = operands
    att_scale = HEAD ** -0.5
    scores = jnp.dot(q_head, k_head.T, preferred_element_type=jnp.float32) * att_scale
    causal = jnp.arange(TOKENS)[:, None] >= jnp.arange(TOKENS)[None, :]
    attn_probs = jax.nn.softmax(jnp.where(causal, scores, -1e30), axis=-1)
    probs_bf = attn_probs.astype(jnp.bfloat16)
    attn_out = jnp.dot(probs_bf, v_head, preferred_element_type=jnp.float32).astype(jnp.bfloat16)
    d_probs = jnp.dot(d_head, v_head.T, preferred_element_type=jnp.float32)
    d_values = jnp.dot(probs_bf.T, d_head, preferred_element_type=jnp.float32)
    row_delta = jnp.sum(attn_probs * d_probs, axis=-1, keepdims=True)
    d_scores = (attn_probs * (d_probs - row_delta) * att_scale).astype(jnp.bfloat16)
    d_q_rot = jnp.dot(d_scores, k_head, preferred_element_type=jnp.float32)
    d_k_rot = jnp.dot(d_scores.T, q_head, preferred_element_type=jnp.float32)
    return attn_out, d_q_rot, d_k_rot, d_values


def reference(resid_x, ln_mean, ln_rstd, ln_gain, grad_y, w_qkv, w_out, w_up, w_down):
    x_hat = (resid_x.astype(jnp.float32) - ln_mean[:, None]) * ln_rstd[:, None]
    gain_f32 = ln_gain.astype(jnp.float32)
    normed = (x_hat * gain_f32).astype(jnp.bfloat16)
    qkv_proj = jnp.dot(normed, w_qkv, preferred_element_type=jnp.float32).reshape(TOKENS, HEADS, 3, HEAD)
    rope_cos, rope_sin = rope_tables()
    q_rot = rotate(qkv_proj[:, :, 0, :], rope_cos, rope_sin).astype(jnp.bfloat16)
    k_rot = rotate(qkv_proj[:, :, 1, :], rope_cos, rope_sin).astype(jnp.bfloat16)
    values = qkv_proj[:, :, 2, :].astype(jnp.bfloat16)
    w_out_rows = w_out.reshape(D, D)
    d_attn = jnp.dot(grad_y, w_out_rows.T, preferred_element_type=jnp.float32).astype(jnp.bfloat16).reshape(TOKENS, HEADS, HEAD)
    head_major = (jnp.transpose(q_rot, (1, 0, 2)), jnp.transpose(k_rot, (1, 0, 2)), jnp.transpose(values, (1, 0, 2)), jnp.transpose(d_attn, (1, 0, 2)))
    head_outs, head_dq, head_dk, head_dv = lax.map(head_pass, head_major)
    attn_out = jnp.transpose(head_outs, (1, 0, 2)).reshape(TOKENS, D)
    d_queries = rotate(jnp.transpose(head_dq, (1, 0, 2)), rope_cos, -rope_sin)
    d_keys = rotate(jnp.transpose(head_dk, (1, 0, 2)), rope_cos, -rope_sin)
    d_values = jnp.transpose(head_dv, (1, 0, 2))
    d_qkv = jnp.stack([d_queries, d_keys, d_values], axis=2).astype(jnp.bfloat16).reshape(TOKENS, 3 * D)
    grad_w_qkv = jnp.dot(normed.T, d_qkv, preferred_element_type=jnp.float32).astype(jnp.bfloat16)
    grad_w_out = jnp.dot(attn_out.T, grad_y, preferred_element_type=jnp.float32).astype(jnp.bfloat16).reshape(HEADS, HEAD, D)
    pre_act = jnp.dot(normed, w_up, preferred_element_type=jnp.float32)
    act_out, gelu_vjp = jax.vjp(exact_gelu, pre_act)
    act_bf = act_out.astype(jnp.bfloat16)
    grad_w_down = jnp.dot(act_bf.T, grad_y, preferred_element_type=jnp.float32).astype(jnp.bfloat16)
    d_act = jnp.dot(grad_y, w_down.T, preferred_element_type=jnp.float32)
    d_pre = gelu_vjp(d_act)[0].astype(jnp.bfloat16)
    grad_w_up = jnp.dot(normed.T, d_pre, preferred_element_type=jnp.float32).astype(jnp.bfloat16)
    d_normed = jnp.dot(d_pre, w_up.T, preferred_element_type=jnp.float32) + jnp.dot(d_qkv, w_qkv.T, preferred_element_type=jnp.float32)
    d_hat = d_normed * gain_f32
    mean_d = jnp.mean(d_hat, axis=1, keepdims=True)
    mean_dx = jnp.mean(d_hat * x_hat, axis=1, keepdims=True)
    grad_x = (grad_y.astype(jnp.float32) + ln_rstd[:, None] * (d_hat - mean_d - x_hat * mean_dx)).astype(jnp.bfloat16)
    return (grad_x, grad_w_qkv, grad_w_out, grad_w_up, grad_w_down)
```

```python
import functools

import jax
import jax.numpy as jnp
from jax import lax
from jax.experimental import pallas as pl
from jax.experimental.pallas import tpu as pltpu
from jax.sharding import PartitionSpec as P

BF = jnp.bfloat16
F32 = jnp.float32
BLK = 512
MLP_ROWS = 256
WG_ROWS = 512
LN_ROWS = 256
CHUNK_BLOCKS = (1, 2, 2, 2, 1)
VMEM_LIMIT = 64 * 1000 * 1024


def dot_nn(a, b):
    return lax.dot_general(a, b, (((1,), (0,)), ((), ())), preferred_element_type=F32)


def dot_nt(a, b):
    return lax.dot_general(a, b, (((1,), (1,)), ((), ())), preferred_element_type=F32)


def dot_tn(a, b):
    return lax.dot_general(a, b, (((0,), (0,)), ((), ())), preferred_element_type=F32)


def column(row):
    return jnp.broadcast_to(row, (128, row.shape[1])).T[:, :1]


def rotate_t(x, cos_t, sin_t):
    half = cos_t.shape[0]
    a, b = x[:half], x[half:2 * half]
    return jnp.concatenate([a * cos_t - b * sin_t, b * cos_t + a * sin_t, x[2 * half:]], axis=0)


def whole(shape, index=None):
    index = index or (0,) * len(shape)
    return pl.BlockSpec(shape, lambda i: index, pipeline_mode=pl.Buffered(1))


ANY = pl.BlockSpec(memory_space=pl.ANY)


def params():
    return pltpu.CompilerParams(dimension_semantics=("arbitrary",), vmem_limit_bytes=VMEM_LIMIT)


def cost(flops, nbytes):
    return pl.CostEstimate(flops=int(flops), bytes_accessed=int(nbytes), transcendentals=0)


def qkv_kernel(x_ref, mean_ref, rstd_ref, g_ref, w_ref, cos_ref, sin_ref, n_ref, q_ref, k_ref, v_ref, kt_ref, vt_ref):
    hd = q_ref.shape[1]
    xh = (x_ref[...].astype(F32) - column(mean_ref[...])) * column(rstd_ref[...])
    n = (xh * g_ref[...].astype(F32)).astype(BF)
    n_ref[...] = n
    proj = dot_nn(n, w_ref[...])
    cos_t, sin_t = cos_ref[...], sin_ref[...]
    q_ref[...] = rotate_t(proj[:, :hd].T, cos_t, sin_t).T.astype(BF)
    kt = rotate_t(proj[:, hd:2 * hd].T, cos_t, sin_t)
    kt_ref[...] = kt.astype(BF)
    k_ref[...] = kt.T.astype(BF)
    v = proj[:, 2 * hd:]
    v_ref[...] = v.astype(BF)
    vt_ref[...] = v.T.astype(BF)


def qkv_call(x, mean, rstd, g, w, cos_t, sin_t):
    t, d = x.shape
    cols = w.shape[1]
    hd = cols // 3
    half = cos_t.shape[0]
    rows = lambda width: pl.BlockSpec((BLK, width), lambda i: (i, 0))
    lanes = lambda height: pl.BlockSpec((height, BLK), lambda i: (0, i))
    sd = lambda *s: jax.ShapeDtypeStruct(s, BF)
    return pl.pallas_call(
        qkv_kernel,
        grid=(t // BLK,),
        in_specs=[rows(d), lanes(1), lanes(1), whole((1, d)), whole((d, cols)), lanes(half), lanes(half)],
        out_specs=[rows(d), rows(hd), rows(hd), rows(hd), lanes(hd), lanes(hd)],
        out_shape=[sd(t, d), sd(t, hd), sd(t, hd), sd(t, hd), sd(hd, t), sd(hd, t)],
        compiler_params=params(),
        cost_estimate=cost(2 * t * d * cols, 4 * t * d),
        name="ln_qkv",
    )(x, mean, rstd, g, w, cos_t, sin_t)


def attn_kernel(top, n_steps, left, has_in, head_dim, *refs):
    n_in = 9 + (4 if has_in else 0)
    ins, rest = refs[:n_in], refs[n_in:]
    q_ref, k_ref, v_ref, kt_ref, vt_ref, dy_ref, wo_ref, cos_ref, sin_ref = ins[:9]
    o_ref, dqkv_ref = rest[:2]
    rest = rest[2:]
    if left:
        dk_out, dv_out = rest[:2]
        rest = rest[2:]
    s_ref, dp_ref, dk_acc, dv_acc, ot_acc, dqt_acc = rest
    step = pl.program_id(0)
    i = top - step
    scale = head_dim ** -0.5
    log2e = 1.4426950408889634

    @pl.when(step == 0)
    def _():
        if has_in:
            dk_acc[...] = ins[9][...]
            dv_acc[...] = ins[10][...]
        else:
            dk_acc[...] = jnp.zeros_like(dk_acc)
            dv_acc[...] = jnp.zeros_like(dv_acc)

    q = q_ref[...]
    d_out = dot_nt(dy_ref[...], wo_ref[0]).astype(BF)
    ot_acc[...] = jnp.zeros_like(ot_acc)
    dqt_acc[...] = jnp.zeros_like(dqt_acc)

    def at(j):
        return pl.ds(pl.multiple_of(j * BLK, BLK), BLK)

    s = dot_nt(k_ref[at(i), :], q) * (scale * log2e)
    key = lax.broadcasted_iota(jnp.int32, (BLK, BLK), 0)
    query = lax.broadcasted_iota(jnp.int32, (BLK, BLK), 1)
    s = jnp.where(key <= query, s, -1e30)
    s_ref[at(i), :] = s
    m = jnp.max(s, axis=0, keepdims=True)
    l = jnp.sum(jnp.exp2(s - m), axis=0, keepdims=True)

    def scores(j, carry):
        m, l = carry
        s = dot_nt(k_ref[at(j), :], q) * (scale * log2e)
        s_ref[at(j), :] = s
        m_new = jnp.maximum(m, jnp.max(s, axis=0, keepdims=True))
        l = l * jnp.exp2(m - m_new) + jnp.sum(jnp.exp2(s - m_new), axis=0, keepdims=True)
        return m_new, l

    m, l = lax.fori_loop(0, i, scores, (m, l))
    m = m + jnp.log2(l)

    def probs(j, delta):
        p = jnp.exp2(s_ref[at(j), :] - m)
        pb = p.astype(BF)
        dp = dot_nt(v_ref[at(j), :], d_out)
        s_ref[at(j), :] = p
        dp_ref[at(j), :] = dp
        dv_acc[at(j), :] += dot_nn(pb, d_out)
        ot_acc[...] += dot_nn(vt_ref[:, at(j)], pb)
        return delta + jnp.sum(p * dp, axis=0, keepdims=True)

    delta = lax.fori_loop(0, i + 1, probs, jnp.zeros((1, BLK), F32))

    def grads(j, carry):
        ds = (s_ref[at(j), :] * (dp_ref[at(j), :] - delta) * scale).astype(BF)
        dk_acc[at(j), :] += dot_nn(ds, q)
        dqt_acc[...] += dot_nn(kt_ref[:, at(j)], ds)
        return carry

    lax.fori_loop(0, i + 1, grads, 0)

    cos_t, sin_t = cos_ref[...], sin_ref[...]
    o_ref[...] = ot_acc[...].T.astype(BF)
    dqkv_ref[:, :head_dim] = rotate_t(dqt_acc[...], cos_t, -sin_t).T.astype(BF)
    dqkv_ref[:, head_dim:2 * head_dim] = rotate_t(dk_acc[at(i), :].T, cos_t, -sin_t).T.astype(BF)
    dqkv_ref[:, 2 * head_dim:] = dv_acc[at(i), :].astype(BF)

    if left:
        @pl.when(step == n_steps - 1)
        def _():
            dk_out[...] = dk_acc[:left, :]
            dv_out[...] = dv_acc[:left, :]


def attn_call(block0, block1, qkv, dy, wo, cos_t, sin_t, carried):
    q, k, v, kt, vt = qkv
    t, hd = q.shape
    d = dy.shape[1]
    half = cos_t.shape[0]
    end, left = block1 * BLK, block0 * BLK
    n_steps = block1 - block0
    top = block1 - 1
    rows = lambda width: pl.BlockSpec((BLK, width), lambda s: (top - s, 0))
    lanes = lambda height: pl.BlockSpec((height, BLK), lambda s: (0, top - s))
    in_specs = [rows(hd), whole((end, hd)), whole((end, hd)), whole((hd, end)), whole((hd, end)), rows(d), whole((1, hd, d)), lanes(half), lanes(half)]
    args = [q, k, v, kt, vt, dy, wo, cos_t, sin_t]
    aliases = {}
    if carried is not None:
        in_specs += [whole((end, hd)), whole((end, hd)), ANY, ANY]
        args += list(carried)
        aliases = {11: 0, 12: 1}
    out_specs = [rows(hd), rows(3 * hd)]
    out_shape = [jax.ShapeDtypeStruct((t, hd), BF), jax.ShapeDtypeStruct((t, 3 * hd), BF)]
    if left:
        out_specs += [whole((left, hd)), whole((left, hd))]
        out_shape += [jax.ShapeDtypeStruct((left, hd), F32)] * 2
    tiles = sum(b + 1 for b in range(block0, block1))
    return pl.pallas_call(
        functools.partial(attn_kernel, top, n_steps, left, carried is not None, hd),
        grid=(n_steps,),
        in_specs=in_specs,
        out_specs=out_specs,
        out_shape=out_shape,
        scratch_shapes=[
            pltpu.VMEM((end, BLK), F32), pltpu.VMEM((end, BLK), F32),
            pltpu.VMEM((end, hd), F32), pltpu.VMEM((end, hd), F32),
            pltpu.VMEM((hd, BLK), F32), pltpu.VMEM((hd, BLK), F32),
        ],
        input_output_aliases=aliases,
        compiler_params=params(),
        cost_estimate=cost(12 * tiles * BLK * BLK * hd * 2, 8 * end * hd),
        name=f"attention_{block0}",
    )(*args)


def mlp_kernel(n_ref, dy_ref, dqkv_ref, w1_ref, w2_ref, wqkv_ref, *refs):
    part_ref, g_ref, da_ref = refs[-3:]
    w1 = w1_ref[...]
    a = dot_nn(n_ref[...], w1)
    dg = dot_nt(dy_ref[...], w2_ref[...])
    cdf = 0.5 * (1.0 + lax.erf(a * 0.7071067811865476))
    g_ref[...] = (a * cdf).astype(BF)
    pdf = jnp.exp(a * a * -0.5) * 0.3989422804014327
    da = (dg * (cdf + a * pdf)).astype(BF)
    da_ref[...] = da
    part_ref[...] = (dot_nt(da, w1) + dot_nt(dqkv_ref[...], wqkv_ref[...])).astype(BF)


def mlp_call(block0, block1, n, dy, dqkv, w1, w2, wqkv, carried):
    t, d = n.shape
    ff = w1.shape[1]
    cols = wqkv.shape[1]
    per = BLK // MLP_ROWS
    first, steps = block0 * per, (block1 - block0) * per
    rows = lambda width: pl.BlockSpec((MLP_ROWS, width), lambda s: (first + s, 0))
    in_specs = [rows(d), rows(d), rows(cols), whole((d, ff)), whole((ff, d)), whole((d, cols))]
    args = [n, dy, dqkv, w1, w2, wqkv]
    aliases = {}
    if carried is not None:
        in_specs += [ANY, ANY]
        args += list(carried)
        aliases = {6: 1, 7: 2}
    size = (block1 - block0) * BLK
    return pl.pallas_call(
        mlp_kernel,
        grid=(steps,),
        in_specs=in_specs,
        out_specs=[pl.BlockSpec((MLP_ROWS, d), lambda s: (s, 0)), rows(ff), rows(ff)],
        out_shape=[jax.ShapeDtypeStruct((size, d), BF), jax.ShapeDtypeStruct((t, ff), BF), jax.ShapeDtypeStruct((t, ff), BF)],
        input_output_aliases=aliases,
        compiler_params=params(),
        cost_estimate=cost(2 * size * d * (3 * ff + cols), 6 * size * d),
        name=f"mlp_{block0}",
    )(*args)


def wgrad_down_kernel(dy_ref, g_ref, o_ref, w2_out, wo_out, acc2, acco):
    step = pl.program_id(0)

    @pl.when(step == 0)
    def _():
        acc2[...] = jnp.zeros_like(acc2)
        acco[...] = jnp.zeros_like(acco)

    dy = dy_ref[...]
    acc2[...] += dot_tn(g_ref[...], dy)
    acco[...] += dot_tn(o_ref[...], dy)

    @pl.when(step == pl.num_programs(0) - 1)
    def _():
        w2_out[...] = acc2[...].astype(BF)
        wo_out[0] = acco[...].astype(BF)


def wgrad_up_kernel(n_ref, da_ref, dqkv_ref, w1_out, wqkv_out, acc1, accq):
    step = pl.program_id(0)

    @pl.when(step == 0)
    def _():
        acc1[...] = jnp.zeros_like(acc1)
        accq[...] = jnp.zeros_like(accq)

    def part(c, carry):
        at = pl.ds(pl.multiple_of(c * 512, 512), 512)
        n = n_ref[:, at]
        acc1[at, :] += dot_tn(n, da_ref[...])
        accq[at, :] += dot_tn(n, dqkv_ref[...])
        return carry

    lax.fori_loop(0, acc1.shape[0] // 512, part, 0)

    @pl.when(step == pl.num_programs(0) - 1)
    def _():
        w1_out[...] = acc1[...].astype(BF)
        wqkv_out[...] = accq[...].astype(BF)


def wgrad_call(kernel, big, left, right, shapes, name):
    t = big.shape[0]
    rows = lambda a: pl.BlockSpec((WG_ROWS, a.shape[1]), lambda i: (i, 0))
    flat = [s[-2:] for s in shapes]
    return pl.pallas_call(
        kernel,
        grid=(t // WG_ROWS,),
        in_specs=[rows(big), rows(left), rows(right)],
        out_specs=[whole(s) for s in shapes],
        out_shape=[jax.ShapeDtypeStruct(s, BF) for s in shapes],
        scratch_shapes=[pltpu.VMEM(s, F32) for s in flat],
        compiler_params=params(),
        cost_estimate=cost(2 * t * big.shape[1] * (left.shape[1] + right.shape[1]), 4 * t * big.shape[1]),
        name=name,
    )(big, left, right)


def ln_kernel(dn_ref, x_ref, dy_ref, mean_ref, rstd_ref, g_ref, *refs):
    out_ref = refs[-1]
    rstd = column(rstd_ref[...])
    xh = (x_ref[...].astype(F32) - column(mean_ref[...])) * rstd
    d = dn_ref[...].astype(F32) * g_ref[...].astype(F32)
    inv = 1.0 / d.shape[1]
    mean_d = jnp.sum(d, axis=1, keepdims=True) * inv
    mean_dx = jnp.sum(d * xh, axis=1, keepdims=True) * inv
    out_ref[...] = (dy_ref[...].astype(F32) + rstd * (d - mean_d - xh * mean_dx)).astype(BF)


def ln_call(block0, block1, dn, x, dy, mean, rstd, g, carried, after):
    t, d = x.shape
    per = BLK // LN_ROWS
    first, steps = block0 * per, (block1 - block0) * per
    rows = pl.BlockSpec((LN_ROWS, d), lambda s: (first + s, 0))
    lanes = pl.BlockSpec((1, LN_ROWS), lambda s: (0, first + s))
    in_specs = [pl.BlockSpec((LN_ROWS, d), lambda s: (s, 0)), rows, rows, lanes, lanes, whole((1, d))]
    args = [dn, x, dy, mean, rstd, g]
    aliases = {}
    if carried is not None:
        in_specs += [ANY]
        args += [carried]
        aliases = {6: 0}
    in_specs += [ANY] * len(after)
    args += list(after)
    return pl.pallas_call(
        ln_kernel,
        grid=(steps,),
        in_specs=in_specs,
        out_specs=rows,
        out_shape=jax.ShapeDtypeStruct((t, d), BF),
        input_output_aliases=aliases,
        compiler_params=params(),
        cost_estimate=cost(20 * dn.shape[0] * d, 8 * dn.shape[0] * d),
        name=f"ln_backward_{block0}",
    )(*args)


def solution(mesh):
    def device_step(resid_x, ln_mean, ln_rstd, ln_gain, grad_y, w_qkv, w_out, w_up, w_down):
        n_model = mesh.shape["model"]
        tokens, d = resid_x.shape
        hd = w_out.shape[1]
        rot = hd // 4
        positions = jnp.arange(tokens, dtype=F32)[None, :]
        inv_freq = jnp.power(10000.0, -2.0 * jnp.arange(rot // 2, dtype=F32) / rot)
        angles = positions * inv_freq[:, None]
        cos_t, sin_t = jnp.cos(angles), jnp.sin(angles)
        mean, rstd, gain = ln_mean[None, :], ln_rstd[None, :], ln_gain[None, :]

        normed, *qkv = qkv_call(resid_x, mean, rstd, gain, w_qkv, cos_t, sin_t)

        bounds = []
        top = tokens // BLK
        for size in CHUNK_BLOCKS:
            bounds.append((top - size, top))
            top -= size
        assert top == 0
        carried, mlp_carried, sums = None, None, []
        for block0, block1 in bounds:
            o, dqkv, *acc = attn_call(block0, block1, qkv, grad_y, w_out, cos_t, sin_t, carried)
            carried = (*acc, o, dqkv)
            part, act, d_pre = mlp_call(block0, block1, normed, grad_y, dqkv, w_up, w_down, w_qkv, mlp_carried)
            mlp_carried = (act, d_pre)
            sums.append(lax.psum(part, "model", axis_index_groups=[[(r + len(sums)) % n_model for r in range(n_model)]]))

        ff = w_up.shape[1]
        grad_w_down, grad_w_out = wgrad_call(wgrad_down_kernel, grad_y, act, o, [(ff, d), (1, hd, d)], "wgrad_down")
        grad_w_up, grad_w_qkv = wgrad_call(wgrad_up_kernel, normed, d_pre, dqkv, [(d, ff), (d, 3 * hd)], "wgrad_up")

        grad_x = None
        after = [grad_w_down, grad_w_up]
        for (block0, block1), dn in zip(bounds, sums):
            grad_x = ln_call(block0, block1, dn, resid_x, grad_y, mean, rstd, gain, grad_x, after)
            after = []
        return grad_x, grad_w_qkv, grad_w_out, grad_w_up, grad_w_down

    in_specs = (P("data", None), P("data"), P("data"), P(None), P("data", None), P(None, "model"), P("model", None, None), P(None, "model"), P("model", None))
    out_specs = (P("data", None), P("data", "model"), P(("data", "model"), None, None), P("data", "model"), P(("data", "model"), None))
    return jax.shard_map(device_step, mesh=mesh, in_specs=in_specs, out_specs=out_specs, check_vma=False)
```

```python
import functools

import jax
import jax.numpy as jnp
from jax import lax
from jax.experimental import pallas as pl
from jax.experimental.pallas import tpu as pltpu
from jax.sharding import PartitionSpec as P

BF = jnp.bfloat16
F32 = jnp.float32
BLK = 512
VMEM_LIMIT = 67043328
MESH = pl.DeviceIdType.MESH
CORES = 2
LOG2E = 1.4426950408889634


def dot_nn(a, b):
    return lax.dot_general(a, b, (((1,), (0,)), ((), ())), preferred_element_type=F32)


def dot_nt(a, b):
    return lax.dot_general(a, b, (((1,), (1,)), ((), ())), preferred_element_type=F32)


def dot_tn(a, b):
    return lax.dot_general(a, b, (((0,), (0,)), ((), ())), preferred_element_type=F32)


def column(row):
    return jnp.broadcast_to(row, (128, row.shape[1])).T[:, :1]


def rotate_t(x, cos_t, sin_t):
    half = cos_t.shape[0]
    a, b = x[:half], x[half:2 * half]
    return jnp.concatenate([a * cos_t - b * sin_t, b * cos_t + a * sin_t, x[2 * half:]], axis=0)


def whole(shape, index=None):
    index = index or (0,) * len(shape)
    return pl.BlockSpec(shape, lambda i: index, pipeline_mode=pl.Buffered(1))


ANY = pl.BlockSpec(memory_space=pl.ANY)


def params():
    return pltpu.CompilerParams(dimension_semantics=("arbitrary",), vmem_limit_bytes=VMEM_LIMIT)


def cost(flops, nbytes):
    return pl.CostEstimate(flops=int(flops), bytes_accessed=int(nbytes), transcendentals=0)


def qkv_kernel(x_ref, mean_ref, rstd_ref, g_ref, w_ref, cos_ref, sin_ref, n_ref, q_ref, k_ref, v_ref, kt_ref, vt_ref, stat_ref):
    hd = q_ref.shape[1]
    mean, rstd = column(mean_ref[...]), column(rstd_ref[...])
    lane = lax.broadcasted_iota(jnp.int32, stat_ref.shape, 1)
    stat_ref[...] = jnp.where(lane == 0, mean, rstd)
    xh = (x_ref[...].astype(F32) - mean) * rstd
    n = (xh * g_ref[...].astype(F32)).astype(BF)
    n_ref[...] = n
    proj = dot_nn(n, w_ref[...])
    cos_t, sin_t = cos_ref[...], sin_ref[...]
    q_ref[...] = rotate_t(proj[:, :hd].T, cos_t, sin_t).T.astype(BF)
    kt = rotate_t(proj[:, hd:2 * hd].T, cos_t, sin_t)
    kt_ref[...] = kt.astype(BF)
    k_ref[...] = kt.T.astype(BF)
    v = proj[:, 2 * hd:]
    v_ref[...] = v.astype(BF)
    vt_ref[...] = v.T.astype(BF)


def qkv_call(x, mean, rstd, g, w, cos_t, sin_t):
    t, d = x.shape
    cols = w.shape[1]
    hd = cols // 3
    half = cos_t.shape[0]
    rows = lambda width: pl.BlockSpec((BLK, width), lambda i: (i, 0))
    lanes = lambda height: pl.BlockSpec((height, BLK), lambda i: (0, i))
    sd = lambda *s: jax.ShapeDtypeStruct(s, BF)
    return pl.pallas_call(
        qkv_kernel,
        grid=(t // BLK,),
        in_specs=[rows(d), lanes(1), lanes(1), whole((1, d)), whole((d, cols)), lanes(half), lanes(half)],
        out_specs=[rows(d), rows(hd), rows(hd), rows(hd), lanes(hd), lanes(hd), rows(128)],
        out_shape=[sd(t, d), sd(t, hd), sd(t, hd), sd(t, hd), sd(hd, t), sd(hd, t), jax.ShapeDtypeStruct((t, 128), F32)],
        compiler_params=params(),
        cost_estimate=cost(2 * t * d * cols, 4 * t * d),
        name="ln_qkv",
    )(x, mean, rstd, g, w, cos_t, sin_t)


def layer_kernel(
    nb, nz, q_ref, k_ref, v_ref, kt_ref, vt_ref, dy_ref, n_ref, cos_ref, sin_ref, wo_ref, w1_ref, w2_ref, wqkv_ref, gain_ref, x_hbm, dy_hbm, stat_hbm,
    dx_hbm, gw1_hbm, gwqkv_hbm, gw2_hbm, gwo_hbm,
    s_ref, dk_acc, dv_acc, ot_acc, dqt_acc, d_out_ref, row_ref, o_ref, dqkv_ref, act_ref, da_ref, acc1, accq, acc2, acco,
    part, pair, stage, recv, shard, x_rows, dy_rows, stat_rows,
    pair_send, pair_recv, rs_send, rs_recv, ag_send, ag_recv, fin_send, fin_recv, load_sem, own_sem, out_sem, credit,
):
    hd = q_ref.shape[1]
    scale = hd ** -0.5
    half = BLK // CORES
    piece = half // nz
    hops = nz // 2
    g = pl.program_id(0)
    i = nb - 1 - g

    me = lax.axis_index("model")
    z, c = lax.div(me, CORES), lax.rem(me, CORES)
    sgn = 1 - 2 * c
    signs = (sgn, -sgn)
    wrap = lambda n: lax.rem(n + 2 * nz, nz)
    partner = z * CORES + (1 - c)
    toward = tuple(wrap(z + s) * CORES + c for s in signs)
    compute, reducing, gathering = g < nb, (g >= 1) & (g <= nb), g >= 2
    red_row = (nb - g) * BLK
    gat_row = (nb + 1 - g) * BLK

    def at(j):
        return pl.ds(pl.multiple_of(j * BLK, BLK), BLK)

    def rows(first, n):
        return pl.ds(pl.multiple_of(first, n), n)

    def remote(src, dst, send_sem, recv_sem, device):
        return pltpu.make_async_remote_copy(src_ref=src, dst_ref=dst, send_sem=send_sem, recv_sem=recv_sem, device_id={"model": device}, device_id_type=MESH)

    def pair_copy():
        return remote(part.at[rows((1 - c) * half, half), :], pair, pair_send, pair_recv, partner)

    def rs_copy(flow, s):
        return remote(stage.at[flow, s - 1], recv.at[flow, s - 1], rs_send.at[flow, s - 1], rs_recv.at[flow, s - 1], toward[flow])

    def mine(p):
        own = part[rows(c * half + p * piece, piece), :].astype(F32)
        return own + pair[rows(p * piece, piece), :].astype(F32)

    def rs_start(flow, s, prior):
        total = mine(wrap(z + signs[flow] * (hops + 1 - s)))
        if prior:
            total += recv[flow, s - 2].astype(F32)
        stage[flow, s - 1] = total.astype(BF)
        rs_copy(flow, s).start()

    def ag_rows(flow, back):
        return rows(gat_row + c * half + wrap(z - signs[flow] * back) * piece, piece)

    def ag_copy(flow, s):
        there = dx_hbm.at[ag_rows(flow, s - 1), :]
        return remote(shard if s == 1 else there, there, ag_send.at[flow, s - 1], ag_recv.at[flow, s - 1], toward[flow])

    def ag_wait(flow, s):
        ag_copy(flow, s).wait_send()
        here = dx_hbm.at[ag_rows(flow, s), :]
        remote(here, here, ag_send.at[flow, s - 1], ag_recv.at[flow, s - 1], toward[flow]).wait_recv()

    def fin_copy(core):
        block = dx_hbm.at[rows(gat_row + core * half, half), :]
        return remote(block, block, fin_send, fin_recv, partner)

    def own_rows(first):
        return rows(first + c * half + z * piece, piece)

    def loads():
        at_rows = own_rows(red_row)
        return [pltpu.make_async_copy(src.at[at_rows, :], dst, load_sem.at[n]) for n, (src, dst) in enumerate(((x_hbm, x_rows), (dy_hbm, dy_rows), (stat_hbm, stat_rows)))]

    def own_store(first):
        return pltpu.make_async_copy(shard, dx_hbm.at[own_rows(first), :], own_sem)

    def weight_stores():
        pairs = ((acc1, gw1_hbm), (accq, gwqkv_hbm), (acc2, gw2_hbm), (acco, gwo_hbm))
        return [pltpu.make_async_copy(src, dst, out_sem.at[n]) for n, (src, dst) in enumerate(pairs)]

    def tick(t):
        if t == 0:
            @pl.when(g >= 1)
            def _():
                pl.semaphore_wait(credit, 3)

            @pl.when(reducing)
            def _():
                pair_copy().start()
                for load in loads():
                    load.start()

            @pl.when(gathering)
            def _():
                for flow in range(2):
                    ag_copy(flow, 1).start()
        elif t % 2 == 1 and t <= 2 * hops - 1:
            s = (t + 1) // 2
            @pl.when(reducing)
            def _():
                if s == 1:
                    pair_copy().wait()
                else:
                    rs_copy(0, s - 1).wait()
                    if s > 2:
                        rs_copy(1, s - 1).wait()
                rs_start(0, s, s > 1)
                if s > 1:
                    rs_start(1, s, s > 2)
        elif t % 2 == 0 and t <= 2 * hops:
            s = t // 2
            @pl.when(gathering)
            def _():
                ag_wait(0, s)
                if s < hops:
                    ag_wait(1, s)
                if s < hops:
                    ag_copy(0, s + 1).start()
                    if s + 1 < hops:
                        ag_copy(1, s + 1).start()
                else:
                    own_store(gat_row).wait()
                    fin_copy(c).start()
        elif t == 2 * hops + 1:
            @pl.when(gathering)
            def _():
                fin_copy(c).wait_send()
                fin_copy(1 - c).wait_recv()

            @pl.when(reducing)
            def _():
                for flow in range(2):
                    rs_copy(flow, hops).wait()
                for load in loads():
                    load.wait()
                total = mine(z) + recv[0, hops - 1].astype(F32) + recv[1, hops - 1].astype(F32)
                d = total * gain_ref[...].astype(F32)
                rstd = stat_rows[:, 1:2]
                xh = (x_rows[...].astype(F32) - stat_rows[:, 0:1]) * rstd
                inv = 1.0 / d.shape[1]
                mean_d = jnp.sum(d, axis=1, keepdims=True) * inv
                mean_dx = jnp.sum(d * xh, axis=1, keepdims=True) * inv
                shard[...] = (dy_rows[...].astype(F32) + rstd * (d - mean_d - xh * mean_dx)).astype(BF)
                own_store(red_row).start()

            @pl.when(g <= nb)
            def _():
                for device in (partner, *toward):
                    pl.semaphore_signal(credit, inc=1, device_id={"model": device}, device_id_type=MESH)

    def scores():
        d_out_ref[...] = dot_nt(dy_ref[...], wo_ref[0]).astype(BF)
        ot_acc[...] = jnp.zeros_like(ot_acc)
        dqt_acc[...] = jnp.zeros_like(dqt_acc)
        q = q_ref[...]
        s = dot_nt(k_ref[at(i), :], q) * (scale * LOG2E)
        key = lax.broadcasted_iota(jnp.int32, (BLK, BLK), 0)
        query = lax.broadcasted_iota(jnp.int32, (BLK, BLK), 1)
        s = jnp.where(key <= query, s, -1e30)
        s_ref[at(i), :] = s
        m = jnp.max(s, axis=0, keepdims=True)
        l = jnp.sum(jnp.exp2(s - m), axis=0, keepdims=True)

        def step(j, carry):
            m, l = carry
            s = dot_nt(k_ref[at(j), :], q) * (scale * LOG2E)
            s_ref[at(j), :] = s
            m_new = jnp.maximum(m, jnp.max(s, axis=0, keepdims=True))
            l = l * jnp.exp2(m - m_new) + jnp.sum(jnp.exp2(s - m_new), axis=0, keepdims=True)
            return m_new, l

        m, l = lax.fori_loop(0, i, step, (m, l))
        row_ref[0:1, :] = m + jnp.log2(l)

    def probs(first, last):
        m = row_ref[0:1, :]

        def step(j, carry):
            pb = jnp.exp2(s_ref[at(j), :] - m).astype(BF)
            dv_acc[at(j), :] += dot_nn(pb, d_out_ref[...])
            ot_acc[...] += dot_nn(vt_ref[:, at(j)], pb)
            return carry

        lax.fori_loop(first, last, step, 0)

    def delta():
        row_ref[1:2, :] = jnp.sum(ot_acc[...] * d_out_ref[...].astype(F32).T, axis=0, keepdims=True)
        o_ref[...] = ot_acc[...].T.astype(BF)

    def grads(first, last):
        m, delta = row_ref[0:1, :], row_ref[1:2, :]

        def step(j, carry):
            dp = dot_nt(v_ref[at(j), :], d_out_ref[...])
            p = jnp.exp2(s_ref[at(j), :] - m)
            ds = (p * (dp - delta) * scale).astype(BF)
            dk_acc[at(j), :] += dot_nn(ds, q_ref[...])
            dqt_acc[...] += dot_nn(kt_ref[:, at(j)], ds)
            return carry

        lax.fori_loop(first, last, step, 0)

    def heads_done():
        cos_t, sin_t = cos_ref[...], sin_ref[...]
        dqkv_ref[:, :hd] = rotate_t(dqt_acc[...], cos_t, -sin_t).T.astype(BF)
        dqkv_ref[:, hd:2 * hd] = rotate_t(dk_acc[at(i), :].T, cos_t, -sin_t).T.astype(BF)
        dqkv_ref[:, 2 * hd:] = dv_acc[at(i), :].astype(BF)

    def mlp(h):
        r = slice(h * half, (h + 1) * half)
        a = dot_nn(n_ref[r, :], w1_ref[...])
        dg = dot_nt(dy_ref[r, :], w2_ref[...])
        cdf = 0.5 * (1.0 + lax.erf(a * 0.7071067811865476))
        act_ref[r, :] = (a * cdf).astype(BF)
        pdf = jnp.exp(a * a * -0.5) * 0.3989422804014327
        da_ref[r, :] = (dg * (cdf + a * pdf)).astype(BF)

    def wgrad_down():
        def step(n, carry):
            cols = rows(n * 512, 512)
            dy = dy_ref[:, cols]
            acc2[:, cols] += dot_tn(act_ref[...], dy)
            acco[:, cols] += dot_tn(o_ref[...], dy)
            return carry

        lax.fori_loop(0, acc2.shape[1] // 512, step, 0)

    def wgrad_up():
        def step(n, carry):
            down = rows(n * 512, 512)
            x = n_ref[:, down]
            acc1[down, :] += dot_tn(x, da_ref[...])
            accq[down, :] += dot_tn(x, dqkv_ref[...])
            return carry

        lax.fori_loop(0, acc1.shape[0] // 512, step, 0)

    def partial_dn():
        for h in range(CORES):
            r = slice(h * half, (h + 1) * half)
            part[r, :] = (dot_nt(da_ref[r, :], w1_ref[...]) + dot_nt(dqkv_ref[r, :], wqkv_ref[...])).astype(BF)

    @pl.when(g == 0)
    def _():
        barrier = pltpu.get_barrier_semaphore()
        for device in (partner, *toward):
            pl.semaphore_signal(barrier, inc=1, device_id={"model": device}, device_id_type=MESH)
        pl.semaphore_wait(barrier, 3)
        for ref in (dk_acc, dv_acc, acc1, accq, acc2, acco):
            ref[...] = jnp.zeros_like(ref)

    @pl.when(g == nb)
    def _():
        for store in weight_stores():
            store.start()

    middle = lax.div(i + 1, 2)
    pieces = (
        lambda: scores(),
        lambda: probs(0, middle),
        lambda: (probs(middle, i + 1), delta()),
        lambda: grads(0, middle),
        lambda: (grads(middle, i + 1), heads_done()),
        lambda: mlp(0),
        lambda: mlp(1),
        lambda: wgrad_down(),
        lambda: wgrad_up(),
        lambda: partial_dn(),
    )
    for t, work in enumerate(pieces):
        tick(t)

        @pl.when(compute)
        def _():
            work()

    @pl.when(g == nb + 1)
    def _():
        for store in weight_stores():
            store.wait()


def layer_call(mesh, qkv, stat, x, n, dy, wo, w1, w2, wqkv, gain, cos_t, sin_t):
    q, k, v, kt, vt = qkv
    t, hd = q.shape
    d = dy.shape[1]
    ff, cols = w1.shape[1], wqkv.shape[1]
    nb = t // BLK
    nz = mesh.shape["model"] // CORES
    rot = cos_t.shape[0]
    half = BLK // CORES
    piece = half // nz
    hops = nz // 2
    block = lambda g: jnp.maximum(nb - 1 - g, 0)
    rows = lambda width: pl.BlockSpec((BLK, width), lambda g: (block(g), 0))
    lanes = lambda height: pl.BlockSpec((height, BLK), lambda g: (0, block(g)))
    vm = pltpu.VMEM
    dma = pltpu.SemaphoreType.DMA
    return pl.pallas_call(
        functools.partial(layer_kernel, nb, nz),
        grid=(nb + 2,),
        in_specs=[rows(hd), whole((t, hd)), whole((t, hd)), whole((hd, t)), whole((hd, t)), rows(d), rows(d), lanes(rot), lanes(rot),
                  whole((1, hd, d)), whole((d, ff)), whole((ff, d)), whole((d, cols)), whole((1, d)), ANY, ANY, ANY],
        out_specs=[ANY] * 5,
        out_shape=[jax.ShapeDtypeStruct((t, d), BF)] + [jax.ShapeDtypeStruct(s, F32) for s in ((d, ff), (d, cols), (ff, d), (hd, d))],
        scratch_shapes=[
            vm((t, BLK), F32), vm((t, hd), F32), vm((t, hd), F32), vm((hd, BLK), F32), vm((hd, BLK), F32),
            vm((BLK, hd), BF), vm((8, BLK), F32), vm((BLK, hd), BF), vm((BLK, cols), BF), vm((BLK, ff), BF), vm((BLK, ff), BF),
            vm((d, ff), F32), vm((d, cols), F32), vm((ff, d), F32), vm((hd, d), F32),
            vm((BLK, d), BF), vm((half, d), BF), vm((2, hops, piece, d), BF), vm((2, hops, piece, d), BF), vm((piece, d), BF),
            vm((piece, d), BF), vm((piece, d), BF), vm((piece, 128), F32),
            dma, dma, dma((2, hops)), dma((2, hops)), dma((2, hops)), dma((2, hops)), dma, dma, dma((3,)), dma, dma((4,)),
            pltpu.SemaphoreType.REGULAR,
        ],
        compiler_params=pltpu.CompilerParams(dimension_semantics=("arbitrary",), vmem_limit_bytes=VMEM_LIMIT, collective_id=0, has_side_effects=True),
        cost_estimate=cost(2 * t * d * (5 * ff + 3 * cols), 12 * t * d),
        name="layer_backward",
    )(q, k, v, kt, vt, dy, n, cos_t, sin_t, wo, w1, w2, wqkv, gain, x, dy, stat)


def solution(mesh):
    def device_step(resid_x, ln_mean, ln_rstd, ln_gain, grad_y, w_qkv, w_out, w_up, w_down):
        tokens, d = resid_x.shape
        hd = w_out.shape[1]
        rot = hd // 4
        positions = jnp.arange(tokens, dtype=F32)[None, :]
        inv_freq = jnp.power(10000.0, -2.0 * jnp.arange(rot // 2, dtype=F32) / rot)
        angles = positions * inv_freq[:, None]
        cos_t, sin_t = jnp.cos(angles), jnp.sin(angles)
        mean, rstd, gain = ln_mean[None, :], ln_rstd[None, :], ln_gain[None, :]
        normed, *qkv, stat = qkv_call(resid_x, mean, rstd, gain, w_qkv, cos_t, sin_t)
        grad_x, gw_up, gw_qkv, gw_down, gw_out = layer_call(mesh, qkv, stat, resid_x, normed, grad_y, w_out, w_up, w_down, w_qkv, gain, cos_t, sin_t)
        return grad_x, gw_qkv.astype(BF), gw_out[None].astype(BF), gw_up.astype(BF), gw_down.astype(BF)

    in_specs = (P("data", None), P("data"), P("data"), P(None), P("data", None), P(None, "model"), P("model", None, None), P(None, "model"), P("model", None))
    out_specs = (P("data", None), P("data", "model"), P(("data", "model"), None, None), P("data", "model"), P(("data", "model"), None))
    return jax.shard_map(device_step, mesh=mesh, in_specs=in_specs, out_specs=out_specs, check_vma=False)
```

```python
import functools

import jax
import jax.numpy as jnp
from jax import lax
from jax.experimental import pallas as pl
from jax.experimental.pallas import tpu as pltpu
from jax.sharding import PartitionSpec as P

BF = jnp.bfloat16
F32 = jnp.float32
BLK = 512
VMEM_LIMIT = 67043328
MESH = pl.DeviceIdType.MESH
CORES = 2
LOG2E = 1.4426950408889634
TICKS = 10
OFFSET = 3


def dot_nn(a, b):
    return lax.dot_general(a, b, (((1,), (0,)), ((), ())), preferred_element_type=F32)


def dot_nt(a, b):
    return lax.dot_general(a, b, (((1,), (1,)), ((), ())), preferred_element_type=F32)


def dot_tn(a, b):
    return lax.dot_general(a, b, (((0,), (0,)), ((), ())), preferred_element_type=F32)


def column(row):
    return jnp.broadcast_to(row, (128, row.shape[1])).T[:, :1]


def rotate_t(x, cos_t, sin_t):
    half = cos_t.shape[0]
    a, b = x[:half], x[half:2 * half]
    return jnp.concatenate([a * cos_t - b * sin_t, b * cos_t + a * sin_t, x[2 * half:]], axis=0)


def whole(shape, index=None):
    index = index or (0,) * len(shape)
    return pl.BlockSpec(shape, lambda i: index, pipeline_mode=pl.Buffered(1))


ANY = pl.BlockSpec(memory_space=pl.ANY)


def params():
    return pltpu.CompilerParams(dimension_semantics=("arbitrary",), vmem_limit_bytes=VMEM_LIMIT)


def cost(flops, nbytes):
    return pl.CostEstimate(flops=int(flops), bytes_accessed=int(nbytes), transcendentals=0)


def qkv_kernel(x_ref, mean_ref, rstd_ref, g_ref, w_ref, cos_ref, sin_ref, n_ref, q_ref, k_ref, v_ref, kt_ref, vt_ref, stat_ref):
    hd = q_ref.shape[1]
    mean, rstd = column(mean_ref[...]), column(rstd_ref[...])
    lane = lax.broadcasted_iota(jnp.int32, stat_ref.shape, 1)
    stat_ref[...] = jnp.where(lane == 0, mean, rstd)
    xh = (x_ref[...].astype(F32) - mean) * rstd
    n = (xh * g_ref[...].astype(F32)).astype(BF)
    n_ref[...] = n
    proj = dot_nn(n, w_ref[...])
    cos_t, sin_t = cos_ref[...], sin_ref[...]
    q_ref[...] = rotate_t(proj[:, :hd].T, cos_t, sin_t).T.astype(BF)
    kt = rotate_t(proj[:, hd:2 * hd].T, cos_t, sin_t)
    kt_ref[...] = kt.astype(BF)
    k_ref[...] = kt.T.astype(BF)
    v = proj[:, 2 * hd:]
    v_ref[...] = v.astype(BF)
    vt_ref[...] = v.T.astype(BF)


def qkv_call(x, mean, rstd, g, w, cos_t, sin_t):
    t, d = x.shape
    cols = w.shape[1]
    hd = cols // 3
    half = cos_t.shape[0]
    rows = lambda width: pl.BlockSpec((BLK, width), lambda i: (i, 0))
    lanes = lambda height: pl.BlockSpec((height, BLK), lambda i: (0, i))
    sd = lambda *s: jax.ShapeDtypeStruct(s, BF)
    return pl.pallas_call(
        qkv_kernel,
        grid=(t // BLK,),
        in_specs=[rows(d), lanes(1), lanes(1), whole((1, d)), whole((d, cols)), lanes(half), lanes(half)],
        out_specs=[rows(d), rows(hd), rows(hd), rows(hd), lanes(hd), lanes(hd), rows(128)],
        out_shape=[sd(t, d), sd(t, hd), sd(t, hd), sd(t, hd), sd(hd, t), sd(hd, t), jax.ShapeDtypeStruct((t, 128), F32)],
        compiler_params=params(),
        cost_estimate=cost(2 * t * d * cols, 4 * t * d),
        name="ln_qkv",
    )(x, mean, rstd, g, w, cos_t, sin_t)


def layer_kernel(
    nb, nz, q_ref, k_ref, v_ref, kt_ref, vt_ref, dy_ref, n_ref, cos_ref, sin_ref, wo_ref, w1_ref, w2_ref, wqkv_ref, gain_ref, x_hbm, dy_hbm, stat_hbm,
    dx_hbm, gw1_hbm, gwqkv_hbm, gw2_hbm, gwo_hbm,
    s_ref, dk_acc, dv_acc, ot_acc, dqt_acc, d_out_ref, row_ref, o_ref, dqkv_ref, act_ref, da_ref, acc1, accq, acc2, acco, wo_cast,
    part, pair, stage, recv, shards, x_rows, dy_rows, stat_rows,
    pair_send, pair_recv, rs_send, rs_recv, ag_send, ag_recv, fin_send, fin_recv, load_sem, own_sem, out_sem, credit,
):
    hd = q_ref.shape[1]
    scale = hd ** -0.5
    sub = BLK // 2
    quarter = sub // CORES
    piece = quarter // nz
    hops = nz // 2
    g = pl.program_id(0)
    i = jnp.maximum(nb - 1 - g, 0)

    me = lax.axis_index("model")
    z, c = lax.div(me, CORES), lax.rem(me, CORES)
    sgn = 1 - 2 * c
    signs = (sgn, -sgn)
    wrap = lambda n: lax.rem(n + 2 * nz, nz)
    partner = z * CORES + (1 - c)
    toward = tuple(wrap(z + s) * CORES + c for s in signs)
    compute = g < nb

    def at(j):
        return pl.ds(pl.multiple_of(j * BLK, BLK), BLK)

    def rows(first, n):
        return pl.ds(pl.multiple_of(first, n), n)

    def remote(src, dst, send_sem, recv_sem, device):
        return pltpu.make_async_remote_copy(src_ref=src, dst_ref=dst, send_sem=send_sem, recv_sem=recv_sem, device_id={"model": device}, device_id_type=MESH)

    def stream(h, t, ge):
        reducing, gathering = (ge >= 1) & (ge <= nb), (ge >= 2) & (ge <= nb + 1)
        red_row = (nb - ge) * BLK + h * sub
        gat_row = (nb + 1 - ge) * BLK + h * sub

        def pair_copy():
            return remote(part.at[rows(h * sub + (1 - c) * quarter, quarter), :], pair.at[h], pair_send.at[h], pair_recv.at[h], partner)

        def rs_copy(flow, s):
            return remote(stage.at[h, flow, s - 1], recv.at[h, flow, s - 1], rs_send.at[h, flow, s - 1], rs_recv.at[h, flow, s - 1], toward[flow])

        def mine(p):
            own = part[rows(h * sub + c * quarter + p * piece, piece), :].astype(F32)
            return own + pair[h, rows(p * piece, piece), :].astype(F32)

        def rs_start(flow, s, prior):
            total = mine(wrap(z + signs[flow] * (hops + 1 - s)))
            if prior:
                total += recv[h, flow, s - 2].astype(F32)
            stage[h, flow, s - 1] = total.astype(BF)
            rs_copy(flow, s).start()

        def shard(flow, back):
            return shards.at[h, rows(wrap(z - signs[flow] * back) * piece, piece), :]

        def ag_copy(flow, s):
            there = shard(flow, s - 1)
            return remote(there, there, ag_send.at[h, flow, s - 1], ag_recv.at[h, flow, s - 1], toward[flow])

        def ag_wait(flow, s):
            ag_copy(flow, s).wait_send()
            here = shard(flow, s)
            remote(here, here, ag_send.at[h, flow, s - 1], ag_recv.at[h, flow, s - 1], toward[flow]).wait_recv()

        def fin_copy(core):
            block = dx_hbm.at[rows(gat_row + core * quarter, quarter), :]
            return remote(shards.at[h], block, fin_send.at[h], fin_recv.at[h], partner)

        def own_store():
            return pltpu.make_async_copy(shards.at[h], dx_hbm.at[rows(gat_row + c * quarter, quarter), :], own_sem.at[h])

        def loads():
            at_rows = rows(red_row + c * quarter + z * piece, piece)
            pairs = ((x_hbm, x_rows), (dy_hbm, dy_rows), (stat_hbm, stat_rows))
            return [pltpu.make_async_copy(src.at[at_rows, :], dst.at[h], load_sem.at[h, n]) for n, (src, dst) in enumerate(pairs)]

        if t == 0:
            @pl.when((ge >= 1) & (ge <= nb + 1))
            def _():
                pl.semaphore_wait(credit.at[h], 3)

            @pl.when(reducing)
            def _():
                pair_copy().start()
                for load in loads():
                    load.start()

            @pl.when(gathering)
            def _():
                for flow in range(2):
                    ag_copy(flow, 1).start()
        elif t % 2 == 1 and t <= 2 * hops - 1:
            s = (t + 1) // 2

            @pl.when(reducing)
            def _():
                if s == 1:
                    pair_copy().wait()
                else:
                    rs_copy(0, s - 1).wait()
                    if s > 2:
                        rs_copy(1, s - 1).wait()
                rs_start(0, s, s > 1)
                if s > 1:
                    rs_start(1, s, s > 2)
        elif t % 2 == 0 and t <= 2 * hops:
            s = t // 2

            @pl.when(gathering)
            def _():
                ag_wait(0, s)
                if s < hops:
                    ag_wait(1, s)
                    ag_copy(0, s + 1).start()
                    if s + 1 < hops:
                        ag_copy(1, s + 1).start()
                else:
                    fin_copy(c).start()
                    own_store().start()
        elif t == 2 * hops + 1:
            @pl.when(gathering)
            def _():
                fin_copy(c).wait_send()
                own_store().wait()
                fin_copy(1 - c).wait_recv()

            @pl.when(reducing)
            def _():
                for flow in range(2):
                    rs_copy(flow, hops).wait()
                for load in loads():
                    load.wait()
                total = mine(z) + recv[h, 0, hops - 1].astype(F32) + recv[h, 1, hops - 1].astype(F32)
                d = total * gain_ref[...].astype(F32)
                rstd = stat_rows[h, :, 1:2]
                xh = (x_rows[h].astype(F32) - stat_rows[h, :, 0:1]) * rstd
                inv = 1.0 / d.shape[1]
                mean_d = jnp.sum(d, axis=1, keepdims=True) * inv
                mean_dx = jnp.sum(d * xh, axis=1, keepdims=True) * inv
                shards[h, rows(z * piece, piece), :] = (dy_rows[h].astype(F32) + rstd * (d - mean_d - xh * mean_dx)).astype(BF)

            @pl.when((ge >= 0) & (ge <= nb))
            def _():
                for device in (partner, *toward):
                    pl.semaphore_signal(credit.at[h], inc=1, device_id={"model": device}, device_id_type=MESH)

    def tick(t):
        stream(0, t, g)
        if t >= OFFSET:
            stream(1, t - OFFSET, g)
        else:
            stream(1, t - OFFSET + TICKS, g - 1)

    def weight_stores(n):
        at_rows = rows(n * 512, 512)
        pairs = ((act_ref, gw1_hbm.at[at_rows, :]), (dqkv_ref, gwqkv_hbm.at[at_rows, :]), (da_ref, gw2_hbm.at[:, at_rows]), (wo_cast, gwo_hbm.at[0, :, at_rows]))
        return [pltpu.make_async_copy(src, dst, out_sem.at[m]) for m, (src, dst) in enumerate(pairs)]

    def weights_out(n):
        if n:
            for store in weight_stores(n - 1):
                store.wait()
        if n < acc1.shape[0] // 512:
            at_rows = rows(n * 512, 512)
            act_ref[...] = acc1[at_rows, :].astype(BF)
            dqkv_ref[...] = accq[at_rows, :].astype(BF)
            da_ref[...] = acc2[:, at_rows].astype(BF)
            wo_cast[...] = acco[:, at_rows].astype(BF)
            for store in weight_stores(n):
                store.start()

    def scores():
        d_out_ref[...] = dot_nt(dy_ref[...], wo_ref[0]).astype(BF)
        ot_acc[...] = jnp.zeros_like(ot_acc)
        dqt_acc[...] = jnp.zeros_like(dqt_acc)
        q = q_ref[...]
        s = dot_nt(k_ref[at(i), :], q) * (scale * LOG2E)
        key = lax.broadcasted_iota(jnp.int32, (BLK, BLK), 0)
        query = lax.broadcasted_iota(jnp.int32, (BLK, BLK), 1)
        s = jnp.where(key <= query, s, -1e30)
        s_ref[at(i), :] = s
        m = jnp.max(s, axis=0, keepdims=True)
        l = jnp.sum(jnp.exp2(s - m), axis=0, keepdims=True)

        def step(j, carry):
            m, l = carry
            s = dot_nt(k_ref[at(j), :], q) * (scale * LOG2E)
            s_ref[at(j), :] = s
            m_new = jnp.maximum(m, jnp.max(s, axis=0, keepdims=True))
            l = l * jnp.exp2(m - m_new) + jnp.sum(jnp.exp2(s - m_new), axis=0, keepdims=True)
            return m_new, l

        m, l = lax.fori_loop(0, i, step, (m, l))
        row_ref[0:1, :] = m + jnp.log2(l)

    def probs(first, last):
        m = row_ref[0:1, :]

        def step(j, carry):
            pb = jnp.exp2(s_ref[at(j), :] - m).astype(BF)
            dv_acc[at(j), :] += dot_nn(pb, d_out_ref[...])
            ot_acc[...] += dot_nn(vt_ref[:, at(j)], pb)
            return carry

        lax.fori_loop(first, last, step, 0)

    def delta():
        row_ref[1:2, :] = jnp.sum(ot_acc[...] * d_out_ref[...].astype(F32).T, axis=0, keepdims=True)
        o_ref[...] = ot_acc[...].T.astype(BF)

    def grads(first, last):
        m, delta = row_ref[0:1, :], row_ref[1:2, :]

        def step(j, carry):
            dp = dot_nt(v_ref[at(j), :], d_out_ref[...])
            p = jnp.exp2(s_ref[at(j), :] - m)
            ds = (p * (dp - delta) * scale).astype(BF)
            dk_acc[at(j), :] += dot_nn(ds, q_ref[...])
            dqt_acc[...] += dot_nn(kt_ref[:, at(j)], ds)
            return carry

        lax.fori_loop(first, last, step, 0)

    def heads_done():
        cos_t, sin_t = cos_ref[...], sin_ref[...]
        dqkv_ref[:, :hd] = rotate_t(dqt_acc[...], cos_t, -sin_t).T.astype(BF)
        dqkv_ref[:, hd:2 * hd] = rotate_t(dk_acc[at(i), :].T, cos_t, -sin_t).T.astype(BF)
        dqkv_ref[:, 2 * hd:] = dv_acc[at(i), :].astype(BF)

    def mlp(h):
        r = slice(h * sub, (h + 1) * sub)
        a = dot_nn(n_ref[r, :], w1_ref[...])
        dg = dot_nt(dy_ref[r, :], w2_ref[...])
        cdf = 0.5 * (1.0 + lax.erf(a * 0.7071067811865476))
        act_ref[r, :] = (a * cdf).astype(BF)
        pdf = jnp.exp(a * a * -0.5) * 0.3989422804014327
        da_ref[r, :] = (dg * (cdf + a * pdf)).astype(BF)

    def wgrad_down():
        def step(n, carry):
            cols = rows(n * 512, 512)
            dy = dy_ref[:, cols]
            acc2[:, cols] += dot_tn(act_ref[...], dy)
            acco[:, cols] += dot_tn(o_ref[...], dy)
            return carry

        lax.fori_loop(0, acc2.shape[1] // 512, step, 0)

    def wgrad_up():
        def step(n, carry):
            down = rows(n * 512, 512)
            x = n_ref[:, down]
            acc1[down, :] += dot_tn(x, da_ref[...])
            accq[down, :] += dot_tn(x, dqkv_ref[...])
            return carry

        lax.fori_loop(0, acc1.shape[0] // 512, step, 0)

    def partial_dn(h):
        r = slice(h * sub, (h + 1) * sub)
        part[r, :] = (dot_nt(da_ref[r, :], w1_ref[...]) + dot_nt(dqkv_ref[r, :], wqkv_ref[...])).astype(BF)

    @pl.when(g == 0)
    def _():
        barrier = pltpu.get_barrier_semaphore()
        for device in (partner, *toward):
            pl.semaphore_signal(barrier, inc=1, device_id={"model": device}, device_id_type=MESH)
        pl.semaphore_wait(barrier, 3)
        for ref in (dk_acc, dv_acc, acc1, accq, acc2, acco):
            ref[...] = jnp.zeros_like(ref)

    middle = lax.div(i + 1, 2)
    pieces = (
        lambda: scores(),
        lambda: probs(0, middle),
        lambda: (probs(middle, i + 1), delta()),
        lambda: grads(0, middle),
        lambda: (grads(middle, i + 1), heads_done()),
        lambda: mlp(0),
        lambda: mlp(1),
        lambda: wgrad_down(),
        lambda: wgrad_up(),
        lambda: partial_dn(0),
    )
    n_out = acc1.shape[0] // 512
    for t, work in enumerate(pieces):
        tick(t)
        if t == OFFSET - 1:
            @pl.when((g >= 1) & (g <= nb))
            def _():
                partial_dn(1)

        @pl.when(compute)
        def _():
            work()

        if OFFSET <= t <= OFFSET + n_out:
            @pl.when(g == nb)
            def _():
                weights_out(t - OFFSET)


def layer_call(mesh, qkv, stat, x, n, dy, wo, w1, w2, wqkv, gain, cos_t, sin_t):
    q, k, v, kt, vt = qkv
    t, hd = q.shape
    d = dy.shape[1]
    ff, cols = w1.shape[1], wqkv.shape[1]
    nb = t // BLK
    nz = mesh.shape["model"] // CORES
    rot = cos_t.shape[0]
    sub = BLK // 2
    quarter = sub // CORES
    piece = quarter // nz
    hops = nz // 2
    block = lambda g: jnp.maximum(nb - 1 - g, 0)
    rows = lambda width: pl.BlockSpec((BLK, width), lambda g: (block(g), 0))
    lanes = lambda height: pl.BlockSpec((height, BLK), lambda g: (0, block(g)))
    vm = pltpu.VMEM
    dma = pltpu.SemaphoreType.DMA
    return pl.pallas_call(
        functools.partial(layer_kernel, nb, nz),
        grid=(nb + 3,),
        in_specs=[rows(hd), whole((t, hd)), whole((t, hd)), whole((hd, t)), whole((hd, t)), rows(d), rows(d), lanes(rot), lanes(rot),
                  whole((1, hd, d)), whole((d, ff)), whole((ff, d)), whole((d, cols)), whole((1, d)), ANY, ANY, ANY],
        out_specs=[ANY] * 5,
        out_shape=[jax.ShapeDtypeStruct(s, BF) for s in ((t, d), (d, ff), (d, cols), (ff, d), (1, hd, d))],
        scratch_shapes=[
            vm((t, BLK), F32), vm((t, hd), F32), vm((t, hd), F32), vm((hd, BLK), F32), vm((hd, BLK), F32),
            vm((BLK, hd), BF), vm((8, BLK), F32), vm((BLK, hd), BF), vm((BLK, cols), BF), vm((BLK, ff), BF), vm((BLK, ff), BF),
            vm((d, ff), F32), vm((d, cols), F32), vm((ff, d), F32), vm((hd, d), F32), vm((hd, 512), BF),
            vm((BLK, d), BF), vm((2, quarter, d), BF), vm((2, 2, hops, piece, d), BF), vm((2, 2, hops, piece, d), BF), vm((2, quarter, d), BF),
            vm((2, piece, d), BF), vm((2, piece, d), BF), vm((2, piece, 128), F32),
            dma((2,)), dma((2,)), dma((2, 2, hops)), dma((2, 2, hops)), dma((2, 2, hops)), dma((2, 2, hops)), dma((2,)), dma((2,)), dma((2, 3)), dma((2,)), dma((4,)),
            pltpu.SemaphoreType.REGULAR((2,)),
        ],
        compiler_params=pltpu.CompilerParams(dimension_semantics=("arbitrary",), vmem_limit_bytes=VMEM_LIMIT, collective_id=0, has_side_effects=True),
        cost_estimate=cost(2 * t * d * (5 * ff + 3 * cols), 12 * t * d),
        name="layer_backward",
    )(q, k, v, kt, vt, dy, n, cos_t, sin_t, wo, w1, w2, wqkv, gain, x, dy, stat)


def solution(mesh):
    def device_step(resid_x, ln_mean, ln_rstd, ln_gain, grad_y, w_qkv, w_out, w_up, w_down):
        tokens, d = resid_x.shape
        hd = w_out.shape[1]
        rot = hd // 4
        positions = jnp.arange(tokens, dtype=F32)[None, :]
        inv_freq = jnp.power(10000.0, -2.0 * jnp.arange(rot // 2, dtype=F32) / rot)
        angles = positions * inv_freq[:, None]
        cos_t, sin_t = jnp.cos(angles), jnp.sin(angles)
        mean, rstd, gain = ln_mean[None, :], ln_rstd[None, :], ln_gain[None, :]
        normed, *qkv, stat = qkv_call(resid_x, mean, rstd, gain, w_qkv, cos_t, sin_t)
        grad_x, gw_up, gw_qkv, gw_down, gw_out = layer_call(mesh, qkv, stat, resid_x, normed, grad_y, w_out, w_up, w_down, w_qkv, gain, cos_t, sin_t)
        return grad_x, gw_qkv, gw_out, gw_up, gw_down

    in_specs = (P("data", None), P("data"), P("data"), P(None), P("data", None), P(None, "model"), P("model", None, None), P(None, "model"), P("model", None))
    out_specs = (P("data", None), P("data", "model"), P(("data", "model"), None, None), P("data", "model"), P(("data", "model"), None))
    return jax.shard_map(device_step, mesh=mesh, in_specs=in_specs, out_specs=out_specs, check_vma=False)
```

```python
import functools

import jax
import jax.numpy as jnp
from jax import lax
from jax.experimental import pallas as pl
from jax.experimental.pallas import tpu as pltpu
from jax.sharding import PartitionSpec as P

BF = jnp.bfloat16
F32 = jnp.float32
BLK = 512
VMEM_LIMIT = 67043328
MESH = pl.DeviceIdType.MESH
CORES = 2
LOG2E = 1.4426950408889634
TICKS = 10
OFFSET = 3


def dot_nn(a, b):
    return lax.dot_general(a, b, (((1,), (0,)), ((), ())), preferred_element_type=F32)


def dot_nt(a, b):
    return lax.dot_general(a, b, (((1,), (1,)), ((), ())), preferred_element_type=F32)


def dot_tn(a, b):
    return lax.dot_general(a, b, (((0,), (0,)), ((), ())), preferred_element_type=F32)


def column(row):
    return jnp.broadcast_to(row, (128, row.shape[1])).T[:, :1]


def rotate_t(x, cos_t, sin_t):
    half = cos_t.shape[0]
    a, b = x[:half], x[half:2 * half]
    return jnp.concatenate([a * cos_t - b * sin_t, b * cos_t + a * sin_t, x[2 * half:]], axis=0)


def whole(shape, index=None):
    index = index or (0,) * len(shape)
    return pl.BlockSpec(shape, lambda i: index, pipeline_mode=pl.Buffered(1))


ANY = pl.BlockSpec(memory_space=pl.ANY)


def params():
    return pltpu.CompilerParams(dimension_semantics=("arbitrary",), vmem_limit_bytes=VMEM_LIMIT)


def cost(flops, nbytes):
    return pl.CostEstimate(flops=int(flops), bytes_accessed=int(nbytes), transcendentals=0)


def qkv_kernel(x_ref, mean_ref, rstd_ref, g_ref, w_ref, cos_ref, sin_ref, n_ref, q_ref, k_ref, v_ref, kt_ref, vt_ref, stat_ref):
    hd = q_ref.shape[1]
    gain = g_ref[...].astype(F32)
    for part in range(2):
        r = slice(part * BLK // 2, (part + 1) * BLK // 2)
        mean, rstd = column(mean_ref[:, r]), column(rstd_ref[:, r])
        lane = lax.broadcasted_iota(jnp.int32, (BLK // 2, stat_ref.shape[1]), 1)
        stat_ref[r, :] = jnp.where(lane == 0, mean, rstd)
        n = ((x_ref[r, :].astype(F32) - mean) * rstd * gain).astype(BF)
        n_ref[r, :] = n
        proj = dot_nn(n, w_ref[...])
        cos_t, sin_t = cos_ref[:, r], sin_ref[:, r]
        q_ref[r, :] = rotate_t(proj[:, :hd].T, cos_t, sin_t).T.astype(BF)
        kt = rotate_t(proj[:, hd:2 * hd].T, cos_t, sin_t)
        kt_ref[:, r] = kt.astype(BF)
        k_ref[r, :] = kt.T.astype(BF)
        v = proj[:, 2 * hd:]
        v_ref[r, :] = v.astype(BF)
        vt_ref[:, r] = v.T.astype(BF)


def qkv_call(x, mean, rstd, g, w, cos_t, sin_t):
    t, d = x.shape
    cols = w.shape[1]
    hd = cols // 3
    half = cos_t.shape[0]
    rows = lambda width: pl.BlockSpec((BLK, width), lambda i: (i, 0))
    lanes = lambda height: pl.BlockSpec((height, BLK), lambda i: (0, i))
    sd = lambda *s: jax.ShapeDtypeStruct(s, BF)
    return pl.pallas_call(
        qkv_kernel,
        grid=(t // BLK,),
        in_specs=[rows(d), lanes(1), lanes(1), whole((1, d)), whole((d, cols)), lanes(half), lanes(half)],
        out_specs=[rows(d), rows(hd), rows(hd), rows(hd), lanes(hd), lanes(hd), rows(128)],
        out_shape=[sd(t, d), sd(t, hd), sd(t, hd), sd(t, hd), sd(hd, t), sd(hd, t), jax.ShapeDtypeStruct((t, 128), F32)],
        compiler_params=params(),
        cost_estimate=cost(2 * t * d * cols, 4 * t * d),
        name="ln_qkv",
    )(x, mean, rstd, g, w, cos_t, sin_t)


def layer_kernel(
    nb, nz, q_ref, k_ref, v_ref, kt_ref, vt_ref, dy_ref, n_ref, cos_ref, sin_ref, wo_ref, w1_ref, w2_ref, wqkv_ref, gain_ref, x_hbm, dy_hbm, stat_hbm,
    dx_hbm, gw1_hbm, gwqkv_hbm, gw2_hbm, gwo_hbm,
    s_ref, dk_acc, dv_acc, ot_acc, dqt_acc, d_out_ref, row_ref, o_ref, dqkv_ref, act_ref, da_ref, acc1, accq, acc2, acco, wo_cast,
    part, pair, stage, recv, shards, x_rows, dy_rows, stat_rows,
    pair_send, pair_recv, rs_send, rs_recv, ag_send, ag_recv, fin_send, fin_recv, load_sem, own_sem, out_sem, credit,
):
    hd = q_ref.shape[1]
    scale = hd ** -0.5
    sub = BLK // 2
    quarter = sub // CORES
    piece = quarter // nz
    hops = nz // 2
    g = pl.program_id(0)
    i = jnp.maximum(nb - 1 - g, 0)

    me = lax.axis_index("model")
    z, c = lax.div(me, CORES), lax.rem(me, CORES)
    sgn = 1 - 2 * c
    signs = (sgn, -sgn)
    wrap = lambda n: lax.rem(n + 2 * nz, nz)
    partner = z * CORES + (1 - c)
    toward = tuple(wrap(z + s) * CORES + c for s in signs)
    compute = g < nb

    def at(j):
        return pl.ds(pl.multiple_of(j * BLK, BLK), BLK)

    def rows(first, n):
        return pl.ds(pl.multiple_of(first, n), n)

    def remote(src, dst, send_sem, recv_sem, device):
        return pltpu.make_async_remote_copy(src_ref=src, dst_ref=dst, send_sem=send_sem, recv_sem=recv_sem, device_id={"model": device}, device_id_type=MESH)

    def part_slot(h, b):
        return lax.rem(b + 6, 2) if h == 0 else 2 + lax.rem(b + 6, 3)

    def stream(h, t, b):
        reducing, gathering = (b >= 0) & (b < nb), (b >= 2) & (b < nb + 2)
        red_row = (nb - 1 - b) * BLK + h * sub
        gat_row = (nb + 1 - b) * BLK + h * sub
        held = part_slot(h, b)
        k = 2 * h + lax.rem(b + 6, 2)

        def pair_copy():
            return remote(part.at[held, rows((1 - c) * quarter, quarter), :], pair.at[k], pair_send.at[k], pair_recv.at[k], partner)

        def rs_copy(flow, s):
            return remote(stage.at[k, flow, (s - 1) % 2], recv.at[k, flow, s - 1], rs_send.at[k, flow, s - 1], rs_recv.at[k, flow, s - 1], toward[flow])

        def mine(p):
            own = part[held, rows(c * quarter + p * piece, piece), :].astype(F32)
            return own + pair[k, rows(p * piece, piece), :].astype(F32)

        def rs_start(flow, s, prior):
            total = mine(wrap(z + signs[flow] * (hops + 1 - s)))
            if prior:
                total += recv[k, flow, s - 2].astype(F32)
            stage[k, flow, (s - 1) % 2] = total.astype(BF)
            rs_copy(flow, s).start()

        def shard(flow, back):
            return shards.at[k, rows(wrap(z - signs[flow] * back) * piece, piece), :]

        def ag_copy(flow, s):
            there = shard(flow, s - 1)
            return remote(there, there, ag_send.at[k, flow, s - 1], ag_recv.at[k, flow, s - 1], toward[flow])

        def ag_wait(flow, s):
            ag_copy(flow, s).wait_send()
            here = shard(flow, s)
            remote(here, here, ag_send.at[k, flow, s - 1], ag_recv.at[k, flow, s - 1], toward[flow]).wait_recv()

        def fin_copy(core):
            block = dx_hbm.at[rows(gat_row + core * quarter, quarter), :]
            return remote(shards.at[k], block, fin_send.at[k], fin_recv.at[k], partner)

        def own_store():
            return pltpu.make_async_copy(shards.at[k], dx_hbm.at[rows(gat_row + c * quarter, quarter), :], own_sem.at[k])

        def loads():
            at_rows = rows(red_row + c * quarter + z * piece, piece)
            pairs = ((x_hbm, x_rows), (dy_hbm, dy_rows), (stat_hbm, stat_rows))
            return [pltpu.make_async_copy(src.at[at_rows, :], dst.at[k], load_sem.at[k, n]) for n, (src, dst) in enumerate(pairs)]

        if t == 0:
            @pl.when(gathering)
            def _():
                pl.semaphore_wait(credit.at[k], 3)

            @pl.when(reducing)
            def _():
                pair_copy().start()
                for load in loads():
                    load.start()

            @pl.when(gathering)
            def _():
                for flow in range(2):
                    ag_copy(flow, 1).start()
        elif t % 2 == 1 and t <= 2 * hops - 1:
            s = (t + 1) // 2

            @pl.when(reducing)
            def _():
                if s == 1:
                    pair_copy().wait()
                else:
                    rs_copy(0, s - 1).wait()
                    if s > 2:
                        rs_copy(1, s - 1).wait()
                rs_start(0, s, s > 1)
                if s > 1:
                    rs_start(1, s, s > 2)
        elif t % 2 == 0 and t <= 2 * hops:
            s = t // 2

            @pl.when(gathering)
            def _():
                ag_wait(0, s)
                if s < hops:
                    ag_wait(1, s)
                    ag_copy(0, s + 1).start()
                    if s + 1 < hops:
                        ag_copy(1, s + 1).start()
                else:
                    fin_copy(c).start()
                    own_store().start()
        elif t == 2 * hops + 1:
            @pl.when(gathering)
            def _():
                fin_copy(c).wait_send()
                own_store().wait()
                fin_copy(1 - c).wait_recv()

            @pl.when(reducing)
            def _():
                for flow in range(2):
                    rs_copy(flow, hops).wait()
                for load in loads():
                    load.wait()
                total = mine(z) + recv[k, 0, hops - 1].astype(F32) + recv[k, 1, hops - 1].astype(F32)
                d = total * gain_ref[...].astype(F32)
                rstd = stat_rows[k, :, 1:2]
                xh = (x_rows[k].astype(F32) - stat_rows[k, :, 0:1]) * rstd
                inv = 1.0 / d.shape[1]
                mean_d = jnp.sum(d, axis=1, keepdims=True) * inv
                mean_dx = jnp.sum(d * xh, axis=1, keepdims=True) * inv
                shards[k, rows(z * piece, piece), :] = (dy_rows[k].astype(F32) + rstd * (d - mean_d - xh * mean_dx)).astype(BF)

            @pl.when(reducing)
            def _():
                for device in (partner, *toward):
                    pl.semaphore_signal(credit.at[k], inc=1, device_id={"model": device}, device_id_type=MESH)

    def tick(t):
        for h in range(2):
            late = t - OFFSET * h
            step = g if late >= 0 else g - 1
            late %= TICKS
            if late % 2 == 0:
                stream(h, late // 2, step - 1)
                stream(h, (TICKS + late) // 2, step - 2)

    def weight_stores(n):
        at_rows = rows(n * 512, 512)
        pairs = ((act_ref, gw1_hbm.at[at_rows, :]), (dqkv_ref, gwqkv_hbm.at[at_rows, :]), (da_ref, gw2_hbm.at[:, at_rows]), (wo_cast, gwo_hbm.at[0, :, at_rows]))
        return [pltpu.make_async_copy(src, dst, out_sem.at[m]) for m, (src, dst) in enumerate(pairs)]

    def weights_out(n):
        if n:
            for store in weight_stores(n - 1):
                store.wait()
        if n < acc1.shape[0] // 512:
            at_rows = rows(n * 512, 512)
            act_ref[...] = acc1[at_rows, :].astype(BF)
            dqkv_ref[...] = accq[at_rows, :].astype(BF)
            da_ref[...] = acc2[:, at_rows].astype(BF)
            wo_cast[...] = acco[:, at_rows].astype(BF)
            for store in weight_stores(n):
                store.start()

    def scores():
        d_out_ref[...] = dot_nt(dy_ref[...], wo_ref[0]).astype(BF)
        ot_acc[...] = jnp.zeros_like(ot_acc)
        dqt_acc[...] = jnp.zeros_like(dqt_acc)
        q = q_ref[...]
        s = dot_nt(k_ref[at(i), :], q) * (scale * LOG2E)
        key = lax.broadcasted_iota(jnp.int32, (BLK, BLK), 0)
        query = lax.broadcasted_iota(jnp.int32, (BLK, BLK), 1)
        s = jnp.where(key <= query, s, -1e30)
        s_ref[at(i), :] = s
        m = jnp.max(s, axis=0, keepdims=True)
        l = jnp.sum(jnp.exp2(s - m), axis=0, keepdims=True)

        def step(j, carry):
            m, l = carry
            s = dot_nt(k_ref[at(j), :], q) * (scale * LOG2E)
            s_ref[at(j), :] = s
            m_new = jnp.maximum(m, jnp.max(s, axis=0, keepdims=True))
            l = l * jnp.exp2(m - m_new) + jnp.sum(jnp.exp2(s - m_new), axis=0, keepdims=True)
            return m_new, l

        m, l = lax.fori_loop(0, i, step, (m, l))
        row_ref[0:1, :] = m + jnp.log2(l)

    def probs(first, last):
        m = row_ref[0:1, :]

        def step(j, carry):
            pb = jnp.exp2(s_ref[at(j), :] - m).astype(BF)
            dv_acc[at(j), :] += dot_nn(pb, d_out_ref[...])
            ot_acc[...] += dot_nn(vt_ref[:, at(j)], pb)
            return carry

        lax.fori_loop(first, last, step, 0)

    def delta():
        row_ref[1:2, :] = jnp.sum(ot_acc[...] * d_out_ref[...].astype(F32).T, axis=0, keepdims=True)
        o_ref[...] = ot_acc[...].T.astype(BF)

    def grads(first, last):
        m, delta = row_ref[0:1, :], row_ref[1:2, :]

        def step(j, carry):
            dp = dot_nt(v_ref[at(j), :], d_out_ref[...])
            p = jnp.exp2(s_ref[at(j), :] - m)
            ds = (p * (dp - delta) * scale).astype(BF)
            dk_acc[at(j), :] += dot_nn(ds, q_ref[...])
            dqt_acc[...] += dot_nn(kt_ref[:, at(j)], ds)
            return carry

        lax.fori_loop(first, last, step, 0)

    def heads_done():
        cos_t, sin_t = cos_ref[...], sin_ref[...]
        dqkv_ref[:, :hd] = rotate_t(dqt_acc[...], cos_t, -sin_t).T.astype(BF)
        dqkv_ref[:, hd:2 * hd] = rotate_t(dk_acc[at(i), :].T, cos_t, -sin_t).T.astype(BF)
        dqkv_ref[:, 2 * hd:] = dv_acc[at(i), :].astype(BF)

    def mlp(h):
        width = w1_ref.shape[1] // 2
        at_cols = slice(h * width, (h + 1) * width)
        a = dot_nn(n_ref[...], w1_ref[:, at_cols])
        dg = dot_nt(dy_ref[...], w2_ref[at_cols, :])
        cdf = 0.5 * (1.0 + lax.erf(a * 0.7071067811865476))
        act_ref[:, at_cols] = (a * cdf).astype(BF)
        pdf = jnp.exp(a * a * -0.5) * 0.3989422804014327
        da_ref[:, at_cols] = (dg * (cdf + a * pdf)).astype(BF)

    def wgrad_down():
        def step(n, carry):
            cols = rows(n * 512, 512)
            dy = dy_ref[:, cols]
            acc2[:, cols] += dot_tn(act_ref[...], dy)
            acco[:, cols] += dot_tn(o_ref[...], dy)
            return carry

        lax.fori_loop(0, acc2.shape[1] // 512, step, 0)

    def wgrad_up():
        def step(n, carry):
            down = rows(n * 512, 512)
            x = n_ref[:, down]
            acc1[down, :] += dot_tn(x, da_ref[...])
            accq[down, :] += dot_tn(x, dqkv_ref[...])
            return carry

        lax.fori_loop(0, acc1.shape[0] // 512, step, 0)

    def partial_dn():
        first, second = part_slot(0, g), part_slot(1, g)

        def step(n, carry):
            cols = rows(n * 512, 512)
            dn = (dot_nt(da_ref[...], w1_ref[cols, :]) + dot_nt(dqkv_ref[...], wqkv_ref[cols, :])).astype(BF)
            part[first, :, cols] = dn[:sub]
            part[second, :, cols] = dn[sub:]
            return carry

        lax.fori_loop(0, part.shape[2] // 512, step, 0)

    @pl.when(g == 0)
    def _():
        barrier = pltpu.get_barrier_semaphore()
        for device in (partner, *toward):
            pl.semaphore_signal(barrier, inc=1, device_id={"model": device}, device_id_type=MESH)
        pl.semaphore_wait(barrier, 3)
        for ref in (dk_acc, dv_acc, acc1, accq, acc2, acco):
            ref[...] = jnp.zeros_like(ref)

    middle = lax.div(i + 1, 2)
    pieces = (
        lambda: scores(),
        lambda: probs(0, middle),
        lambda: (probs(middle, i + 1), delta()),
        lambda: grads(0, middle),
        lambda: (grads(middle, i + 1), heads_done()),
        lambda: mlp(0),
        lambda: mlp(1),
        lambda: wgrad_down(),
        lambda: wgrad_up(),
        lambda: partial_dn(),
    )
    n_out = acc1.shape[0] // 512
    for t, work in enumerate(pieces):
        tick(t)

        @pl.when(compute)
        def _():
            work()

        if t <= n_out:
            @pl.when(g == nb)
            def _():
                weights_out(t)


def layer_call(mesh, qkv, stat, x, n, dy, wo, w1, w2, wqkv, gain, cos_t, sin_t):
    q, k, v, kt, vt = qkv
    t, hd = q.shape
    d = dy.shape[1]
    ff, cols = w1.shape[1], wqkv.shape[1]
    nb = t // BLK
    nz = mesh.shape["model"] // CORES
    rot = cos_t.shape[0]
    sub = BLK // 2
    quarter = sub // CORES
    piece = quarter // nz
    hops = nz // 2
    block = lambda g: jnp.maximum(nb - 1 - g, 0)
    rows = lambda width: pl.BlockSpec((BLK, width), lambda g: (block(g), 0))
    lanes = lambda height: pl.BlockSpec((height, BLK), lambda g: (0, block(g)))
    vm = pltpu.VMEM
    dma = pltpu.SemaphoreType.DMA
    return pl.pallas_call(
        functools.partial(layer_kernel, nb, nz),
        grid=(nb + 5,),
        in_specs=[rows(hd), whole((t, hd)), whole((t, hd)), whole((hd, t)), whole((hd, t)), rows(d), rows(d), lanes(rot), lanes(rot),
                  whole((1, hd, d)), whole((d, ff)), whole((ff, d)), whole((d, cols)), whole((1, d)), ANY, ANY, ANY],
        out_specs=[ANY] * 5,
        out_shape=[jax.ShapeDtypeStruct(s, BF) for s in ((t, d), (d, ff), (d, cols), (ff, d), (1, hd, d))],
        scratch_shapes=[
            vm((t, BLK), F32), vm((t, hd), F32), vm((t, hd), F32), vm((hd, BLK), F32), vm((hd, BLK), F32),
            vm((BLK, hd), BF), vm((8, BLK), F32), vm((BLK, hd), BF), vm((BLK, cols), BF), vm((BLK, ff), BF), vm((BLK, ff), BF),
            vm((d, ff), F32), vm((d, cols), F32), vm((ff, d), F32), vm((hd, d), F32), vm((hd, 512), BF),
            vm((5, sub, d), BF), vm((4, quarter, d), BF), vm((4, 2, 2, piece, d), BF), vm((4, 2, hops, piece, d), BF), vm((4, quarter, d), BF),
            vm((4, piece, d), BF), vm((4, piece, d), BF), vm((4, piece, 128), F32),
            dma((4,)), dma((4,)), dma((4, 2, hops)), dma((4, 2, hops)), dma((4, 2, hops)), dma((4, 2, hops)), dma((4,)), dma((4,)), dma((4, 3)), dma((4,)), dma((4,)),
            pltpu.SemaphoreType.REGULAR((4,)),
        ],
        compiler_params=pltpu.CompilerParams(dimension_semantics=("arbitrary",), vmem_limit_bytes=VMEM_LIMIT, collective_id=0, has_side_effects=True),
        cost_estimate=cost(2 * t * d * (5 * ff + 3 * cols), 12 * t * d),
        name="layer_backward",
    )(q, k, v, kt, vt, dy, n, cos_t, sin_t, wo, w1, w2, wqkv, gain, x, dy, stat)


def solution(mesh):
    def device_step(resid_x, ln_mean, ln_rstd, ln_gain, grad_y, w_qkv, w_out, w_up, w_down):
        tokens, d = resid_x.shape
        hd = w_out.shape[1]
        rot = hd // 4
        positions = jnp.arange(tokens, dtype=F32)[None, :]
        inv_freq = jnp.power(10000.0, -2.0 * jnp.arange(rot // 2, dtype=F32) / rot)
        angles = positions * inv_freq[:, None]
        cos_t, sin_t = jnp.cos(angles), jnp.sin(angles)
        mean, rstd, gain = ln_mean[None, :], ln_rstd[None, :], ln_gain[None, :]
        normed, *qkv, stat = qkv_call(resid_x, mean, rstd, gain, w_qkv, cos_t, sin_t)
        grad_x, gw_up, gw_qkv, gw_down, gw_out = layer_call(mesh, qkv, stat, resid_x, normed, grad_y, w_out, w_up, w_down, w_qkv, gain, cos_t, sin_t)
        return grad_x, gw_qkv, gw_out, gw_up, gw_down

    in_specs = (P("data", None), P("data"), P("data"), P(None), P("data", None), P(None, "model"), P("model", None, None), P(None, "model"), P("model", None))
    out_specs = (P("data", None), P("data", "model"), P(("data", "model"), None, None), P("data", "model"), P(("data", "model"), None))
    return jax.shard_map(device_step, mesh=mesh, in_specs=in_specs, out_specs=out_specs, check_vma=False)
```

```python
import functools

import jax
import jax.numpy as jnp
from jax import lax
from jax.experimental import pallas as pl
from jax.experimental.pallas import tpu as pltpu
from jax.sharding import PartitionSpec as P

BF = jnp.bfloat16
F32 = jnp.float32
BLK = 512
VMEM_LIMIT = 67043328
MESH = pl.DeviceIdType.MESH
CORES = 2
LOG2E = 1.4426950408889634
TICKS = 10
PUT_OFF = 2
OFFSET = 3


def dot_nn(a, b):
    return lax.dot_general(a, b, (((1,), (0,)), ((), ())), preferred_element_type=F32)


def dot_nt(a, b):
    return lax.dot_general(a, b, (((1,), (1,)), ((), ())), preferred_element_type=F32)


def dot_tn(a, b):
    return lax.dot_general(a, b, (((0,), (0,)), ((), ())), preferred_element_type=F32)


def column(row):
    return jnp.broadcast_to(row, (128, row.shape[1])).T[:, :1]


def rotate_t(x, cos_t, sin_t):
    half = cos_t.shape[0]
    a, b = x[:half], x[half:2 * half]
    return jnp.concatenate([a * cos_t - b * sin_t, b * cos_t + a * sin_t, x[2 * half:]], axis=0)


def whole(shape, index=None):
    index = index or (0,) * len(shape)
    return pl.BlockSpec(shape, lambda i: index, pipeline_mode=pl.Buffered(1))


ANY = pl.BlockSpec(memory_space=pl.ANY)


def params():
    return pltpu.CompilerParams(dimension_semantics=("arbitrary",), vmem_limit_bytes=VMEM_LIMIT)


def cost(flops, nbytes):
    return pl.CostEstimate(flops=int(flops), bytes_accessed=int(nbytes), transcendentals=0)


def qkv_kernel(x_ref, mean_ref, rstd_ref, g_ref, w_ref, cos_ref, sin_ref, n_ref, q_ref, k_ref, v_ref, kt_ref, vt_ref, stat_ref):
    hd = q_ref.shape[1]
    mean, rstd = column(mean_ref[...]), column(rstd_ref[...])
    lane = lax.broadcasted_iota(jnp.int32, stat_ref.shape, 1)
    stat_ref[...] = jnp.where(lane == 0, mean, rstd)
    xh = (x_ref[...].astype(F32) - mean) * rstd
    n = (xh * g_ref[...].astype(F32)).astype(BF)
    n_ref[...] = n
    proj = dot_nn(n, w_ref[...])
    cos_t, sin_t = cos_ref[...], sin_ref[...]
    q_ref[...] = rotate_t(proj[:, :hd].T, cos_t, sin_t).T.astype(BF)
    kt = rotate_t(proj[:, hd:2 * hd].T, cos_t, sin_t)
    kt_ref[...] = kt.astype(BF)
    k_ref[...] = kt.T.astype(BF)
    v = proj[:, 2 * hd:]
    v_ref[...] = v.astype(BF)
    vt_ref[...] = v.T.astype(BF)


def qkv_call(x, mean, rstd, g, w, cos_t, sin_t):
    t, d = x.shape
    cols = w.shape[1]
    hd = cols // 3
    half = cos_t.shape[0]
    rows = lambda width: pl.BlockSpec((BLK, width), lambda i: (i, 0))
    lanes = lambda height: pl.BlockSpec((height, BLK), lambda i: (0, i))
    sd = lambda *s: jax.ShapeDtypeStruct(s, BF)
    return pl.pallas_call(
        qkv_kernel,
        grid=(t // BLK,),
        in_specs=[rows(d), lanes(1), lanes(1), whole((1, d)), whole((d, cols)), lanes(half), lanes(half)],
        out_specs=[rows(d), rows(hd), rows(hd), rows(hd), lanes(hd), lanes(hd), rows(128)],
        out_shape=[sd(t, d), sd(t, hd), sd(t, hd), sd(t, hd), sd(hd, t), sd(hd, t), jax.ShapeDtypeStruct((t, 128), F32)],
        compiler_params=params(),
        cost_estimate=cost(2 * t * d * cols, 4 * t * d),
        name="ln_qkv",
    )(x, mean, rstd, g, w, cos_t, sin_t)


def layer_kernel(
    nb, nz, q_ref, k_ref, v_ref, kt_ref, vt_ref, dy_ref, n_ref, cos_ref, sin_ref, wo_ref, w1_ref, w2_ref, wqkv_ref, gain_ref, x_hbm, dy_hbm, stat_hbm,
    dx_hbm, gw1_hbm, gwqkv_hbm, gw2_hbm, gwo_hbm,
    s_ref, dk_acc, dv_acc, ot_acc, dqt_acc, d_out_ref, row_ref, o_ref, dqkv_ref, act_ref, da_ref, acc1, accq, acc2, acco, wo_cast,
    part, pair, stage, recv, shards, x_rows, dy_rows, stat_rows,
    pair_send, pair_recv, rs_send, rs_recv, ag_send, ag_recv, fin_send, fin_recv, load_sem, own_sem, out_sem, credit,
):
    hd = q_ref.shape[1]
    scale = hd ** -0.5
    sub = BLK // 2
    quarter = sub // CORES
    piece = quarter // nz
    hops = nz // 2
    g = pl.program_id(0)
    i = jnp.maximum(nb - 1 - g, 0)

    me = lax.axis_index("model")
    z, c = lax.div(me, CORES), lax.rem(me, CORES)
    sgn = 1 - 2 * c
    signs = (sgn, -sgn)
    wrap = lambda n: lax.rem(n + 2 * nz, nz)
    partner = z * CORES + (1 - c)
    toward = tuple(wrap(z + s) * CORES + c for s in signs)
    compute = g < nb
    slot = jnp.minimum(g, PUT_OFF)

    def at(j):
        return pl.ds(pl.multiple_of(j * BLK, BLK), BLK)

    def rows(first, n):
        return pl.ds(pl.multiple_of(first, n), n)

    def remote(src, dst, send_sem, recv_sem, device):
        return pltpu.make_async_remote_copy(src_ref=src, dst_ref=dst, send_sem=send_sem, recv_sem=recv_sem, device_id={"model": device}, device_id_type=MESH)

    def part_slot(h, b):
        return lax.rem(b + 6, 2) if h == 0 else 2 + lax.rem(b + 6, 3)

    def stream(h, t, b):
        reducing, gathering = (b >= 0) & (b < nb), (b >= 2) & (b < nb + 2)
        red_row = (nb - 1 - b) * BLK + h * sub
        gat_row = (nb + 1 - b) * BLK + h * sub
        held = part_slot(h, b)
        k = 2 * h + lax.rem(b + 6, 2)

        def pair_copy():
            return remote(part.at[held, rows((1 - c) * quarter, quarter), :], pair.at[k], pair_send.at[k], pair_recv.at[k], partner)

        def rs_copy(flow, s):
            return remote(stage.at[k, flow, (s - 1) % 2], recv.at[k, flow, s - 1], rs_send.at[k, flow, s - 1], rs_recv.at[k, flow, s - 1], toward[flow])

        def mine(p):
            own = part[held, rows(c * quarter + p * piece, piece), :].astype(F32)
            return own + pair[k, rows(p * piece, piece), :].astype(F32)

        def rs_start(flow, s, prior):
            total = mine(wrap(z + signs[flow] * (hops + 1 - s)))
            if prior:
                total += recv[k, flow, s - 2].astype(F32)
            stage[k, flow, (s - 1) % 2] = total.astype(BF)
            rs_copy(flow, s).start()

        def shard(flow, back):
            return shards.at[k, rows(wrap(z - signs[flow] * back) * piece, piece), :]

        def ag_copy(flow, s):
            there = shard(flow, s - 1)
            return remote(there, there, ag_send.at[k, flow, s - 1], ag_recv.at[k, flow, s - 1], toward[flow])

        def ag_wait(flow, s):
            ag_copy(flow, s).wait_send()
            here = shard(flow, s)
            remote(here, here, ag_send.at[k, flow, s - 1], ag_recv.at[k, flow, s - 1], toward[flow]).wait_recv()

        def fin_copy(core):
            block = dx_hbm.at[rows(gat_row + core * quarter, quarter), :]
            return remote(shards.at[k], block, fin_send.at[k], fin_recv.at[k], partner)

        def own_store():
            return pltpu.make_async_copy(shards.at[k], dx_hbm.at[rows(gat_row + c * quarter, quarter), :], own_sem.at[k])

        def loads():
            at_rows = rows(red_row + c * quarter + z * piece, piece)
            pairs = ((x_hbm, x_rows), (dy_hbm, dy_rows), (stat_hbm, stat_rows))
            return [pltpu.make_async_copy(src.at[at_rows, :], dst.at[k], load_sem.at[k, n]) for n, (src, dst) in enumerate(pairs)]

        if t == 0:
            @pl.when(gathering)
            def _():
                pl.semaphore_wait(credit.at[k], 3)

            @pl.when(reducing)
            def _():
                pair_copy().start()
                for load in loads():
                    load.start()

            @pl.when(gathering)
            def _():
                for flow in range(2):
                    ag_copy(flow, 1).start()
        elif t % 2 == 1 and t <= 2 * hops - 1:
            s = (t + 1) // 2

            @pl.when(reducing)
            def _():
                if s == 1:
                    pair_copy().wait()
                else:
                    rs_copy(0, s - 1).wait()
                    if s > 2:
                        rs_copy(1, s - 1).wait()
                rs_start(0, s, s > 1)
                if s > 1:
                    rs_start(1, s, s > 2)
        elif t % 2 == 0 and t <= 2 * hops:
            s = t // 2

            @pl.when(gathering)
            def _():
                ag_wait(0, s)
                if s < hops:
                    ag_wait(1, s)
                    ag_copy(0, s + 1).start()
                    if s + 1 < hops:
                        ag_copy(1, s + 1).start()
                else:
                    fin_copy(c).start()
                    own_store().start()
        elif t == 2 * hops + 1:
            @pl.when(gathering)
            def _():
                fin_copy(c).wait_send()
                own_store().wait()
                fin_copy(1 - c).wait_recv()

            @pl.when(reducing)
            def _():
                for flow in range(2):
                    rs_copy(flow, hops).wait()
                for load in loads():
                    load.wait()
                total = mine(z) + recv[k, 0, hops - 1].astype(F32) + recv[k, 1, hops - 1].astype(F32)
                d = total * gain_ref[...].astype(F32)
                rstd = stat_rows[k, :, 1:2]
                xh = (x_rows[k].astype(F32) - stat_rows[k, :, 0:1]) * rstd
                inv = 1.0 / d.shape[1]
                mean_d = jnp.sum(d, axis=1, keepdims=True) * inv
                mean_dx = jnp.sum(d * xh, axis=1, keepdims=True) * inv
                shards[k, rows(z * piece, piece), :] = (dy_rows[k].astype(F32) + rstd * (d - mean_d - xh * mean_dx)).astype(BF)

            @pl.when(reducing)
            def _():
                for device in (partner, *toward):
                    pl.semaphore_signal(credit.at[k], inc=1, device_id={"model": device}, device_id_type=MESH)

    def tick(t):
        for h in range(2):
            late = t - OFFSET * h
            step = g if late >= 0 else g - 1
            late %= TICKS
            if late % 2 == 0:
                stream(h, late // 2, step - 1)
                stream(h, (TICKS + late) // 2, step - 2)

    def weight_stores(n):
        at_rows = rows(n * 512, 512)
        pairs = ((act_ref.at[PUT_OFF], gw1_hbm.at[at_rows, :]), (dqkv_ref.at[PUT_OFF], gwqkv_hbm.at[at_rows, :]), (da_ref.at[PUT_OFF], gw2_hbm.at[:, at_rows]), (wo_cast, gwo_hbm.at[0, :, at_rows]))
        return [pltpu.make_async_copy(src, dst, out_sem.at[m]) for m, (src, dst) in enumerate(pairs)]

    def weights_out(n):
        if n:
            for store in weight_stores(n - 1):
                store.wait()
        if n < acc1.shape[0] // 512:
            at_rows = rows(n * 512, 512)
            act_ref[PUT_OFF] = acc1[at_rows, :].astype(BF)
            dqkv_ref[PUT_OFF] = accq[at_rows, :].astype(BF)
            da_ref[PUT_OFF] = acc2[:, at_rows].astype(BF)
            wo_cast[...] = acco[:, at_rows].astype(BF)
            for store in weight_stores(n):
                store.start()

    def scores():
        d_out_ref[...] = dot_nt(dy_ref[...], wo_ref[0]).astype(BF)
        ot_acc[...] = jnp.zeros_like(ot_acc)
        dqt_acc[...] = jnp.zeros_like(dqt_acc)
        q = q_ref[...]
        s = dot_nt(k_ref[at(i), :], q) * (scale * LOG2E)
        key = lax.broadcasted_iota(jnp.int32, (BLK, BLK), 0)
        query = lax.broadcasted_iota(jnp.int32, (BLK, BLK), 1)
        s = jnp.where(key <= query, s, -1e30)
        s_ref[at(i), :] = s
        m = jnp.max(s, axis=0, keepdims=True)
        l = jnp.sum(jnp.exp2(s - m), axis=0, keepdims=True)

        def step(j, carry):
            m, l = carry
            s = dot_nt(k_ref[at(j), :], q) * (scale * LOG2E)
            s_ref[at(j), :] = s
            m_new = jnp.maximum(m, jnp.max(s, axis=0, keepdims=True))
            l = l * jnp.exp2(m - m_new) + jnp.sum(jnp.exp2(s - m_new), axis=0, keepdims=True)
            return m_new, l

        m, l = lax.fori_loop(0, i, step, (m, l))
        row_ref[0:1, :] = m + jnp.log2(l)

    def probs(first, last):
        m = row_ref[0:1, :]

        def step(j, carry):
            pb = jnp.exp2(s_ref[at(j), :] - m).astype(BF)
            dv_acc[at(j), :] += dot_nn(pb, d_out_ref[...])
            ot_acc[...] += dot_nn(vt_ref[:, at(j)], pb)
            return carry

        lax.fori_loop(first, last, step, 0)

    def delta():
        row_ref[1:2, :] = jnp.sum(ot_acc[...] * d_out_ref[...].astype(F32).T, axis=0, keepdims=True)
        o_ref[slot] = ot_acc[...].T.astype(BF)

    def grads(first, last):
        m, delta = row_ref[0:1, :], row_ref[1:2, :]

        def step(j, carry):
            dp = dot_nt(v_ref[at(j), :], d_out_ref[...])
            p = jnp.exp2(s_ref[at(j), :] - m)
            ds = (p * (dp - delta) * scale).astype(BF)
            dk_acc[at(j), :] += dot_nn(ds, q_ref[...])
            dqt_acc[...] += dot_nn(kt_ref[:, at(j)], ds)
            return carry

        lax.fori_loop(first, last, step, 0)

    def heads_done():
        cos_t, sin_t = cos_ref[...], sin_ref[...]
        dqkv_ref[slot, :, :hd] = rotate_t(dqt_acc[...], cos_t, -sin_t).T.astype(BF)
        dqkv_ref[slot, :, hd:2 * hd] = rotate_t(dk_acc[at(i), :].T, cos_t, -sin_t).T.astype(BF)
        dqkv_ref[slot, :, 2 * hd:] = dv_acc[at(i), :].astype(BF)

    def mlp(h):
        width = w1_ref.shape[1] // 2
        at_cols = slice(h * width, (h + 1) * width)
        a = dot_nn(n_ref[...], w1_ref[:, at_cols])
        dg = dot_nt(dy_ref[...], w2_ref[at_cols, :])
        cdf = 0.5 * (1.0 + lax.erf(a * 0.7071067811865476))
        act_ref[slot, :, at_cols] = (a * cdf).astype(BF)
        pdf = jnp.exp(a * a * -0.5) * 0.3989422804014327
        da_ref[slot, :, at_cols] = (dg * (cdf + a * pdf)).astype(BF)

    def down_step(n, used):
        cols = rows(n * 512, 512)
        dy = dy_ref[:, cols]
        acc2[:, cols] += dot_tn(act_ref[used], dy)
        acco[:, cols] += dot_tn(o_ref[used], dy)

    def up_step(n, used):
        down = rows(n * 512, 512)
        x = n_ref[:, down]
        acc1[down, :] += dot_tn(x, da_ref[used])
        accq[down, :] += dot_tn(x, dqkv_ref[used])

    n_out = acc1.shape[0] // 512

    def each(step):
        lax.fori_loop(0, n_out, lambda n, carry: (step(n, PUT_OFF), carry)[1], 0)

    def partial_dn():
        first, second = part_slot(0, g), part_slot(1, g)

        def step(n, carry):
            cols = rows(n * 512, 512)
            dn = (dot_nt(da_ref[slot], w1_ref[cols, :]) + dot_nt(dqkv_ref[slot], wqkv_ref[cols, :])).astype(BF)
            part[first, :, cols] = dn[:sub]
            part[second, :, cols] = dn[sub:]
            return carry

        lax.fori_loop(0, part.shape[2] // 512, step, 0)

    @pl.when(g == 0)
    def _():
        barrier = pltpu.get_barrier_semaphore()
        for device in (partner, *toward):
            pl.semaphore_signal(barrier, inc=1, device_id={"model": device}, device_id_type=MESH)
        pl.semaphore_wait(barrier, 3)
        for ref in (dk_acc, dv_acc, acc1, accq, acc2, acco):
            ref[...] = jnp.zeros_like(ref)

    middle = lax.div(i + 1, 2)
    late = compute & (g >= PUT_OFF)
    pieces = (
        (compute, lambda: scores()),
        (compute, lambda: probs(0, middle)),
        (compute, lambda: (probs(middle, i + 1), delta())),
        (compute, lambda: grads(0, middle)),
        (compute, lambda: (grads(middle, i + 1), heads_done())),
        (compute, lambda: mlp(0)),
        (compute, lambda: mlp(1)),
        (late, lambda: each(down_step)),
        (late, lambda: each(up_step)),
        (compute, lambda: partial_dn()),
    )
    for t, (when, work) in enumerate(pieces):
        tick(t)

        @pl.when(when)
        def _():
            work()

        if t < 2 * n_out:
            @pl.when((g >= nb) & (g < nb + PUT_OFF))
            def _():
                (down_step if t < n_out else up_step)(t % n_out, g - nb)

        if t <= n_out:
            @pl.when(g == nb + PUT_OFF)
            def _():
                weights_out(t)


def layer_call(mesh, qkv, stat, x, n, dy, wo, w1, w2, wqkv, gain, cos_t, sin_t):
    q, k, v, kt, vt = qkv
    t, hd = q.shape
    d = dy.shape[1]
    ff, cols = w1.shape[1], wqkv.shape[1]
    nb = t // BLK
    nz = mesh.shape["model"] // CORES
    rot = cos_t.shape[0]
    sub = BLK // 2
    quarter = sub // CORES
    piece = quarter // nz
    hops = nz // 2
    block = lambda g: jnp.maximum(nb - 1 - g, 0)
    again = lambda g: jnp.where(g < nb, nb - 1 - g, nb - 1 - jnp.minimum(g - nb, PUT_OFF - 1))
    rows = lambda width: pl.BlockSpec((BLK, width), lambda g: (block(g), 0))
    twice = lambda width: pl.BlockSpec((BLK, width), lambda g: (again(g), 0))
    lanes = lambda height: pl.BlockSpec((height, BLK), lambda g: (0, block(g)))
    vm = pltpu.VMEM
    dma = pltpu.SemaphoreType.DMA
    return pl.pallas_call(
        functools.partial(layer_kernel, nb, nz),
        grid=(nb + 5,),
        in_specs=[rows(hd), whole((t, hd)), whole((t, hd)), whole((hd, t)), whole((hd, t)), twice(d), twice(d), lanes(rot), lanes(rot),
                  whole((1, hd, d)), whole((d, ff)), whole((ff, d)), whole((d, cols)), whole((1, d)), ANY, ANY, ANY],
        out_specs=[ANY] * 5,
        out_shape=[jax.ShapeDtypeStruct(s, BF) for s in ((t, d), (d, ff), (d, cols), (ff, d), (1, hd, d))],
        scratch_shapes=[
            vm((t, BLK), F32), vm((t, hd), F32), vm((t, hd), F32), vm((hd, BLK), F32), vm((hd, BLK), F32),
            vm((BLK, hd), BF), vm((8, BLK), F32), vm((PUT_OFF + 1, BLK, hd), BF), vm((PUT_OFF + 1, BLK, cols), BF), vm((PUT_OFF + 1, BLK, ff), BF), vm((PUT_OFF + 1, BLK, ff), BF),
            vm((d, ff), F32), vm((d, cols), F32), vm((ff, d), F32), vm((hd, d), F32), vm((hd, 512), BF),
            vm((5, sub, d), BF), vm((4, quarter, d), BF), vm((4, 2, 2, piece, d), BF), vm((4, 2, hops, piece, d), BF), vm((4, quarter, d), BF),
            vm((4, piece, d), BF), vm((4, piece, d), BF), vm((4, piece, 128), F32),
            dma((4,)), dma((4,)), dma((4, 2, hops)), dma((4, 2, hops)), dma((4, 2, hops)), dma((4, 2, hops)), dma((4,)), dma((4,)), dma((4, 3)), dma((4,)), dma((4,)),
            pltpu.SemaphoreType.REGULAR((4,)),
        ],
        compiler_params=pltpu.CompilerParams(dimension_semantics=("arbitrary",), vmem_limit_bytes=VMEM_LIMIT, collective_id=0, has_side_effects=True),
        cost_estimate=cost(2 * t * d * (5 * ff + 3 * cols), 12 * t * d),
        name="layer_backward",
    )(q, k, v, kt, vt, dy, n, cos_t, sin_t, wo, w1, w2, wqkv, gain, x, dy, stat)


def copy_kernel(*refs):
    n = len(refs) // 2
    for src, dst in zip(refs[:n], refs[n:]):
        dst[...] = src[...]


def copy_call(arrays):
    steps = 8

    def spec(a):
        shape = (*a.shape[:-2], a.shape[-2] // steps, a.shape[-1])
        return pl.BlockSpec(shape, lambda i: (*(0,) * (len(shape) - 2), i, 0))

    specs = [spec(a) for a in arrays]
    return pl.pallas_call(
        copy_kernel,
        grid=(steps,),
        in_specs=specs,
        out_specs=specs,
        out_shape=[jax.ShapeDtypeStruct(a.shape, a.dtype) for a in arrays],
        compiler_params=params(),
        name="results",
    )(*arrays)


def solution(mesh):
    def device_step(resid_x, ln_mean, ln_rstd, ln_gain, grad_y, w_qkv, w_out, w_up, w_down):
        tokens, d = resid_x.shape
        hd = w_out.shape[1]
        rot = hd // 4
        positions = jnp.arange(tokens, dtype=F32)[None, :]
        inv_freq = jnp.power(10000.0, -2.0 * jnp.arange(rot // 2, dtype=F32) / rot)
        angles = positions * inv_freq[:, None]
        cos_t, sin_t = jnp.cos(angles), jnp.sin(angles)
        mean, rstd, gain = ln_mean[None, :], ln_rstd[None, :], ln_gain[None, :]
        normed, *qkv, stat = qkv_call(resid_x, mean, rstd, gain, w_qkv, cos_t, sin_t)
        grad_x, gw_up, gw_qkv, gw_down, gw_out = copy_call(layer_call(mesh, qkv, stat, resid_x, normed, grad_y, w_out, w_up, w_down, w_qkv, gain, cos_t, sin_t))
        return grad_x, gw_qkv, gw_out, gw_up, gw_down

    in_specs = (P("data", None), P("data"), P("data"), P(None), P("data", None), P(None, "model"), P("model", None, None), P(None, "model"), P("model", None))
    out_specs = (P("data", None), P("data", "model"), P(("data", "model"), None, None), P("data", "model"), P(("data", "model"), None))
    return jax.shard_map(device_step, mesh=mesh, in_specs=in_specs, out_specs=out_specs, check_vma=False)
```

```python
import functools

import jax
import jax.numpy as jnp
from jax import lax
from jax.experimental import pallas as pl
from jax.experimental.pallas import tpu as pltpu
from jax.sharding import PartitionSpec as P

BF = jnp.bfloat16
F32 = jnp.float32
BLK = 512
VMEM_LIMIT = 67043328
MESH = pl.DeviceIdType.MESH
CORES = 2
LOG2E = 1.4426950408889634
TICKS = 10
PUT_OFF = 3
OFFSET = 3


def dot_nn(a, b):
    return lax.dot_general(a, b, (((1,), (0,)), ((), ())), preferred_element_type=F32)


def dot_nt(a, b):
    return lax.dot_general(a, b, (((1,), (1,)), ((), ())), preferred_element_type=F32)


def dot_tn(a, b):
    return lax.dot_general(a, b, (((0,), (0,)), ((), ())), preferred_element_type=F32)


def column(row):
    return jnp.broadcast_to(row, (128, row.shape[1])).T[:, :1]


def rotate_t(x, cos_t, sin_t):
    half = cos_t.shape[0]
    a, b = x[:half], x[half:2 * half]
    return jnp.concatenate([a * cos_t - b * sin_t, b * cos_t + a * sin_t, x[2 * half:]], axis=0)


def whole(shape, index=None):
    index = index or (0,) * len(shape)
    return pl.BlockSpec(shape, lambda i: index, pipeline_mode=pl.Buffered(1))


ANY = pl.BlockSpec(memory_space=pl.ANY)


def params():
    return pltpu.CompilerParams(dimension_semantics=("arbitrary",), vmem_limit_bytes=VMEM_LIMIT)


def cost(flops, nbytes):
    return pl.CostEstimate(flops=int(flops), bytes_accessed=int(nbytes), transcendentals=0)


def qkv_kernel(x_ref, mean_ref, rstd_ref, g_ref, w_ref, cos_ref, sin_ref, n_ref, q_ref, k_ref, v_ref, kt_ref, vt_ref, stat_ref):
    hd = q_ref.shape[1]
    mean, rstd = column(mean_ref[...]), column(rstd_ref[...])
    lane = lax.broadcasted_iota(jnp.int32, stat_ref.shape, 1)
    stat_ref[...] = jnp.where(lane == 0, mean, rstd)
    xh = (x_ref[...].astype(F32) - mean) * rstd
    n = (xh * g_ref[...].astype(F32)).astype(BF)
    n_ref[...] = n
    proj = dot_nn(n, w_ref[...])
    cos_t, sin_t = cos_ref[...], sin_ref[...]
    q_ref[...] = rotate_t(proj[:, :hd].T, cos_t, sin_t).T.astype(BF)
    kt = rotate_t(proj[:, hd:2 * hd].T, cos_t, sin_t)
    kt_ref[...] = kt.astype(BF)
    k_ref[...] = kt.T.astype(BF)
    v = proj[:, 2 * hd:]
    v_ref[...] = v.astype(BF)
    vt_ref[...] = v.T.astype(BF)


def qkv_call(x, mean, rstd, g, w, cos_t, sin_t):
    t, d = x.shape
    cols = w.shape[1]
    hd = cols // 3
    half = cos_t.shape[0]
    rows = lambda width: pl.BlockSpec((BLK, width), lambda i: (i, 0))
    lanes = lambda height: pl.BlockSpec((height, BLK), lambda i: (0, i))
    sd = lambda *s: jax.ShapeDtypeStruct(s, BF)
    return pl.pallas_call(
        qkv_kernel,
        grid=(t // BLK,),
        in_specs=[rows(d), lanes(1), lanes(1), whole((1, d)), whole((d, cols)), lanes(half), lanes(half)],
        out_specs=[rows(d), rows(hd), rows(hd), rows(hd), lanes(hd), lanes(hd), rows(128)],
        out_shape=[sd(t, d), sd(t, hd), sd(t, hd), sd(t, hd), sd(hd, t), sd(hd, t), jax.ShapeDtypeStruct((t, 128), F32)],
        compiler_params=params(),
        cost_estimate=cost(2 * t * d * cols, 4 * t * d),
        name="ln_qkv",
    )(x, mean, rstd, g, w, cos_t, sin_t)


def layer_kernel(
    nb, nz, q_ref, k_ref, v_ref, kt_ref, vt_ref, dy_ref, n_ref, cos_ref, sin_ref, wo_ref, w1_ref, w2_ref, wqkv_ref, gain_ref, x_hbm, dy_hbm, stat_hbm,
    dx_hbm, gw1_hbm, gwqkv_hbm, gw2_hbm, gwo_hbm,
    s_ref, dk_acc, dv_acc, ot_acc, dqt_acc, d_out_ref, row_ref, o_ref, dqkv_ref, act_ref, da_ref, acc1, accq, acc2, acco, wo_cast,
    part, pair, stage, recv, shards, x_rows, dy_rows, stat_rows,
    pair_send, pair_recv, rs_send, rs_recv, ag_send, ag_recv, fin_send, fin_recv, load_sem, own_sem, out_sem, credit,
):
    hd = q_ref.shape[1]
    scale = hd ** -0.5
    sub = BLK // 2
    quarter = sub // CORES
    piece = quarter // nz
    hops = nz // 2
    g = pl.program_id(0)
    i = jnp.maximum(nb - 1 - g, 0)

    me = lax.axis_index("model")
    z, c = lax.div(me, CORES), lax.rem(me, CORES)
    sgn = 1 - 2 * c
    signs = (sgn, -sgn)
    wrap = lambda n: lax.rem(n + 2 * nz, nz)
    partner = z * CORES + (1 - c)
    toward = tuple(wrap(z + s) * CORES + c for s in signs)
    compute = g < nb
    slot = jnp.minimum(g, PUT_OFF)

    def at(j):
        return pl.ds(pl.multiple_of(j * BLK, BLK), BLK)

    def rows(first, n):
        return pl.ds(pl.multiple_of(first, n), n)

    def remote(src, dst, send_sem, recv_sem, device):
        return pltpu.make_async_remote_copy(src_ref=src, dst_ref=dst, send_sem=send_sem, recv_sem=recv_sem, device_id={"model": device}, device_id_type=MESH)

    def part_slot(h, b):
        return lax.rem(b + 6, 2) if h == 0 else 2 + lax.rem(b + 6, 3)

    def stream(h, t, b):
        reducing, gathering = (b >= 0) & (b < nb), (b >= 2) & (b < nb + 2)
        red_row = (nb - 1 - b) * BLK + h * sub
        gat_row = (nb + 1 - b) * BLK + h * sub
        held = part_slot(h, b)
        k = 2 * h + lax.rem(b + 6, 2)

        def pair_copy():
            return remote(part.at[held, rows((1 - c) * quarter, quarter), :], pair.at[k], pair_send.at[k], pair_recv.at[k], partner)

        def rs_copy(flow, s):
            return remote(stage.at[k, flow, (s - 1) % 2], recv.at[k, flow, s - 1], rs_send.at[k, flow, s - 1], rs_recv.at[k, flow, s - 1], toward[flow])

        def mine(p):
            own = part[held, rows(c * quarter + p * piece, piece), :].astype(F32)
            return own + pair[k, rows(p * piece, piece), :].astype(F32)

        def rs_start(flow, s, prior):
            total = mine(wrap(z + signs[flow] * (hops + 1 - s)))
            if prior:
                total += recv[k, flow, s - 2].astype(F32)
            stage[k, flow, (s - 1) % 2] = total.astype(BF)
            rs_copy(flow, s).start()

        def shard(flow, back):
            return shards.at[k, rows(wrap(z - signs[flow] * back) * piece, piece), :]

        def ag_copy(flow, s):
            there = shard(flow, s - 1)
            return remote(there, there, ag_send.at[k, flow, s - 1], ag_recv.at[k, flow, s - 1], toward[flow])

        def ag_wait(flow, s):
            ag_copy(flow, s).wait_send()
            here = shard(flow, s)
            remote(here, here, ag_send.at[k, flow, s - 1], ag_recv.at[k, flow, s - 1], toward[flow]).wait_recv()

        def fin_copy(core):
            block = dx_hbm.at[rows(gat_row + core * quarter, quarter), :]
            return remote(shards.at[k], block, fin_send.at[k], fin_recv.at[k], partner)

        def own_store():
            return pltpu.make_async_copy(shards.at[k], dx_hbm.at[rows(gat_row + c * quarter, quarter), :], own_sem.at[k])

        def loads():
            at_rows = rows(red_row + c * quarter + z * piece, piece)
            pairs = ((x_hbm, x_rows), (dy_hbm, dy_rows), (stat_hbm, stat_rows))
            return [pltpu.make_async_copy(src.at[at_rows, :], dst.at[k], load_sem.at[k, n]) for n, (src, dst) in enumerate(pairs)]

        if t == 0:
            @pl.when(gathering)
            def _():
                pl.semaphore_wait(credit.at[k], 3)

            @pl.when(reducing)
            def _():
                pair_copy().start()
                for load in loads():
                    load.start()

            @pl.when(gathering)
            def _():
                for flow in range(2):
                    ag_copy(flow, 1).start()
        elif t % 2 == 1 and t <= 2 * hops - 1:
            s = (t + 1) // 2

            @pl.when(reducing)
            def _():
                if s == 1:
                    pair_copy().wait()
                else:
                    rs_copy(0, s - 1).wait()
                    if s > 2:
                        rs_copy(1, s - 1).wait()
                rs_start(0, s, s > 1)
                if s > 1:
                    rs_start(1, s, s > 2)
        elif t % 2 == 0 and t <= 2 * hops:
            s = t // 2

            @pl.when(gathering)
            def _():
                ag_wait(0, s)
                if s < hops:
                    ag_wait(1, s)
                    ag_copy(0, s + 1).start()
                    if s + 1 < hops:
                        ag_copy(1, s + 1).start()
                else:
                    fin_copy(c).start()
                    own_store().start()
        elif t == 2 * hops + 1:
            @pl.when(gathering)
            def _():
                fin_copy(c).wait_send()
                own_store().wait()
                fin_copy(1 - c).wait_recv()

            @pl.when(reducing)
            def _():
                for flow in range(2):
                    rs_copy(flow, hops).wait()
                for load in loads():
                    load.wait()
                total = mine(z) + recv[k, 0, hops - 1].astype(F32) + recv[k, 1, hops - 1].astype(F32)
                d = total * gain_ref[...].astype(F32)
                rstd = stat_rows[k, :, 1:2]
                xh = (x_rows[k].astype(F32) - stat_rows[k, :, 0:1]) * rstd
                inv = 1.0 / d.shape[1]
                mean_d = jnp.sum(d, axis=1, keepdims=True) * inv
                mean_dx = jnp.sum(d * xh, axis=1, keepdims=True) * inv
                shards[k, rows(z * piece, piece), :] = (dy_rows[k].astype(F32) + rstd * (d - mean_d - xh * mean_dx)).astype(BF)

            @pl.when(reducing)
            def _():
                for device in (partner, *toward):
                    pl.semaphore_signal(credit.at[k], inc=1, device_id={"model": device}, device_id_type=MESH)

    def tick(t):
        for h in range(2):
            late = t - OFFSET * h
            step = g if late >= 0 else g - 1
            late %= TICKS
            if late % 2 == 0:
                stream(h, late // 2, step - 1)
                stream(h, (TICKS + late) // 2, step - 2)

    def weight_stores(n):
        at_rows = rows(n * 512, 512)
        pairs = ((act_ref.at[PUT_OFF], gw1_hbm.at[at_rows, :]), (dqkv_ref.at[PUT_OFF], gwqkv_hbm.at[at_rows, :]), (da_ref.at[PUT_OFF], gw2_hbm.at[:, at_rows]), (wo_cast, gwo_hbm.at[0, :, at_rows]))
        return [pltpu.make_async_copy(src, dst, out_sem.at[m]) for m, (src, dst) in enumerate(pairs)]

    def weights_out(n):
        if n:
            for store in weight_stores(n - 1):
                store.wait()
        if n < acc1.shape[0] // 512:
            at_rows = rows(n * 512, 512)
            act_ref[PUT_OFF] = acc1[at_rows, :].astype(BF)
            dqkv_ref[PUT_OFF] = accq[at_rows, :].astype(BF)
            da_ref[PUT_OFF] = acc2[:, at_rows].astype(BF)
            wo_cast[...] = acco[:, at_rows].astype(BF)
            for store in weight_stores(n):
                store.start()

    def scores():
        d_out_ref[...] = dot_nt(dy_ref[...], wo_ref[0]).astype(BF)
        ot_acc[...] = jnp.zeros_like(ot_acc)
        dqt_acc[...] = jnp.zeros_like(dqt_acc)
        q = q_ref[...]
        s = dot_nt(k_ref[at(i), :], q) * (scale * LOG2E)
        key = lax.broadcasted_iota(jnp.int32, (BLK, BLK), 0)
        query = lax.broadcasted_iota(jnp.int32, (BLK, BLK), 1)
        s = jnp.where(key <= query, s, -1e30)
        s_ref[at(i), :] = s
        m = jnp.max(s, axis=0, keepdims=True)
        l = jnp.sum(jnp.exp2(s - m), axis=0, keepdims=True)

        def step(j, carry):
            m, l = carry
            s = dot_nt(k_ref[at(j), :], q) * (scale * LOG2E)
            s_ref[at(j), :] = s
            m_new = jnp.maximum(m, jnp.max(s, axis=0, keepdims=True))
            l = l * jnp.exp2(m - m_new) + jnp.sum(jnp.exp2(s - m_new), axis=0, keepdims=True)
            return m_new, l

        m, l = lax.fori_loop(0, i, step, (m, l))
        row_ref[0:1, :] = m + jnp.log2(l)

    def probs(first, last):
        m = row_ref[0:1, :]

        def step(j, carry):
            pb = jnp.exp2(s_ref[at(j), :] - m).astype(BF)
            dv_acc[at(j), :] += dot_nn(pb, d_out_ref[...])
            ot_acc[...] += dot_nn(vt_ref[:, at(j)], pb)
            return carry

        lax.fori_loop(first, last, step, 0)

    def delta():
        row_ref[1:2, :] = jnp.sum(ot_acc[...] * d_out_ref[...].astype(F32).T, axis=0, keepdims=True)
        o_ref[slot] = ot_acc[...].T.astype(BF)

    def grads(first, last):
        m, delta = row_ref[0:1, :], row_ref[1:2, :]

        def step(j, carry):
            dp = dot_nt(v_ref[at(j), :], d_out_ref[...])
            p = jnp.exp2(s_ref[at(j), :] - m)
            ds = (p * (dp - delta) * scale).astype(BF)
            dk_acc[at(j), :] += dot_nn(ds, q_ref[...])
            dqt_acc[...] += dot_nn(kt_ref[:, at(j)], ds)
            return carry

        lax.fori_loop(first, last, step, 0)

    def heads_done():
        cos_t, sin_t = cos_ref[...], sin_ref[...]
        dqkv_ref[slot, :, :hd] = rotate_t(dqt_acc[...], cos_t, -sin_t).T.astype(BF)
        dqkv_ref[slot, :, hd:2 * hd] = rotate_t(dk_acc[at(i), :].T, cos_t, -sin_t).T.astype(BF)
        dqkv_ref[slot, :, 2 * hd:] = dv_acc[at(i), :].astype(BF)

    def mlp(h):
        width = w1_ref.shape[1] // 2
        at_cols = slice(h * width, (h + 1) * width)
        a = dot_nn(n_ref[...], w1_ref[:, at_cols])
        dg = dot_nt(dy_ref[...], w2_ref[at_cols, :])
        cdf = 0.5 * (1.0 + lax.erf(a * 0.7071067811865476))
        act_ref[slot, :, at_cols] = (a * cdf).astype(BF)
        pdf = jnp.exp(a * a * -0.5) * 0.3989422804014327
        da_ref[slot, :, at_cols] = (dg * (cdf + a * pdf)).astype(BF)

    def down_step(n, used):
        cols = rows(n * 512, 512)
        dy = dy_ref[:, cols]
        acc2[:, cols] += dot_tn(act_ref[used], dy)
        acco[:, cols] += dot_tn(o_ref[used], dy)

    def up_step(n, used):
        down = rows(n * 512, 512)
        x = n_ref[:, down]
        acc1[down, :] += dot_tn(x, da_ref[used])
        accq[down, :] += dot_tn(x, dqkv_ref[used])

    n_out = acc1.shape[0] // 512

    def each(step):
        lax.fori_loop(0, n_out, lambda n, carry: (step(n, PUT_OFF), carry)[1], 0)

    def partial_dn():
        first, second = part_slot(0, g), part_slot(1, g)

        def step(n, carry):
            cols = rows(n * 512, 512)
            dn = (dot_nt(da_ref[slot], w1_ref[cols, :]) + dot_nt(dqkv_ref[slot], wqkv_ref[cols, :])).astype(BF)
            part[first, :, cols] = dn[:sub]
            part[second, :, cols] = dn[sub:]
            return carry

        lax.fori_loop(0, part.shape[2] // 512, step, 0)

    @pl.when(g == 0)
    def _():
        barrier = pltpu.get_barrier_semaphore()
        for device in (partner, *toward):
            pl.semaphore_signal(barrier, inc=1, device_id={"model": device}, device_id_type=MESH)
        pl.semaphore_wait(barrier, 3)
        for ref in (dk_acc, dv_acc, acc1, accq, acc2, acco):
            ref[...] = jnp.zeros_like(ref)

    middle = lax.div(i + 1, 2)
    late = compute & (g >= PUT_OFF)
    pieces = (
        (compute, lambda: scores()),
        (compute, lambda: probs(0, middle)),
        (compute, lambda: (probs(middle, i + 1), delta())),
        (compute, lambda: grads(0, middle)),
        (compute, lambda: (grads(middle, i + 1), heads_done())),
        (compute, lambda: mlp(0)),
        (compute, lambda: mlp(1)),
        (late, lambda: each(down_step)),
        (late, lambda: each(up_step)),
        (compute, lambda: partial_dn()),
    )
    for t, (when, work) in enumerate(pieces):
        tick(t)

        @pl.when(when)
        def _():
            work()

        if t < 2 * n_out:
            @pl.when((g >= nb) & (g < nb + PUT_OFF))
            def _():
                (down_step if t < n_out else up_step)(t % n_out, g - nb)

        if t <= n_out:
            @pl.when(g == nb + PUT_OFF)
            def _():
                weights_out(t)


def layer_call(mesh, qkv, stat, x, n, dy, wo, w1, w2, wqkv, gain, cos_t, sin_t):
    q, k, v, kt, vt = qkv
    t, hd = q.shape
    d = dy.shape[1]
    ff, cols = w1.shape[1], wqkv.shape[1]
    nb = t // BLK
    nz = mesh.shape["model"] // CORES
    rot = cos_t.shape[0]
    sub = BLK // 2
    quarter = sub // CORES
    piece = quarter // nz
    hops = nz // 2
    block = lambda g: jnp.maximum(nb - 1 - g, 0)
    again = lambda g: jnp.where(g < nb, nb - 1 - g, nb - 1 - jnp.minimum(g - nb, PUT_OFF - 1))
    rows = lambda width: pl.BlockSpec((BLK, width), lambda g: (block(g), 0))
    twice = lambda width: pl.BlockSpec((BLK, width), lambda g: (again(g), 0))
    lanes = lambda height: pl.BlockSpec((height, BLK), lambda g: (0, block(g)))
    vm = pltpu.VMEM
    dma = pltpu.SemaphoreType.DMA
    return pl.pallas_call(
        functools.partial(layer_kernel, nb, nz),
        grid=(nb + 5,),
        in_specs=[rows(hd), whole((t, hd)), whole((t, hd)), whole((hd, t)), whole((hd, t)), twice(d), twice(d), lanes(rot), lanes(rot),
                  whole((1, hd, d)), whole((d, ff)), whole((ff, d)), whole((d, cols)), whole((1, d)), ANY, ANY, ANY],
        out_specs=[ANY] * 5,
        out_shape=[jax.ShapeDtypeStruct(s, BF) for s in ((t, d), (d, ff), (d, cols), (ff, d), (1, hd, d))],
        scratch_shapes=[
            vm((t, BLK), F32), vm((t, hd), F32), vm((t, hd), F32), vm((hd, BLK), F32), vm((hd, BLK), F32),
            vm((BLK, hd), BF), vm((8, BLK), F32), vm((PUT_OFF + 1, BLK, hd), BF), vm((PUT_OFF + 1, BLK, cols), BF), vm((PUT_OFF + 1, BLK, ff), BF), vm((PUT_OFF + 1, BLK, ff), BF),
            vm((d, ff), F32), vm((d, cols), F32), vm((ff, d), F32), vm((hd, d), F32), vm((hd, 512), BF),
            vm((5, sub, d), BF), vm((4, quarter, d), BF), vm((4, 2, 2, piece, d), BF), vm((4, 2, hops, piece, d), BF), vm((4, quarter, d), BF),
            vm((4, piece, d), BF), vm((4, piece, d), BF), vm((4, piece, 128), F32),
            dma((4,)), dma((4,)), dma((4, 2, hops)), dma((4, 2, hops)), dma((4, 2, hops)), dma((4, 2, hops)), dma((4,)), dma((4,)), dma((4, 3)), dma((4,)), dma((4,)),
            pltpu.SemaphoreType.REGULAR((4,)),
        ],
        compiler_params=pltpu.CompilerParams(dimension_semantics=("arbitrary",), vmem_limit_bytes=VMEM_LIMIT, collective_id=0, has_side_effects=True),
        cost_estimate=cost(2 * t * d * (5 * ff + 3 * cols), 12 * t * d),
        name="layer_backward",
    )(q, k, v, kt, vt, dy, n, cos_t, sin_t, wo, w1, w2, wqkv, gain, x, dy, stat)


def copy_kernel(*refs):
    n = len(refs) // 2
    for src, dst in zip(refs[:n], refs[n:]):
        dst[...] = src[...]


def copy_call(arrays):
    steps = 8

    def spec(a):
        shape = (*a.shape[:-2], a.shape[-2] // steps, a.shape[-1])
        return pl.BlockSpec(shape, lambda i: (*(0,) * (len(shape) - 2), i, 0))

    specs = [spec(a) for a in arrays]
    return pl.pallas_call(
        copy_kernel,
        grid=(steps,),
        in_specs=specs,
        out_specs=specs,
        out_shape=[jax.ShapeDtypeStruct(a.shape, a.dtype) for a in arrays],
        compiler_params=params(),
        name="results",
    )(*arrays)


def solution(mesh):
    def device_step(resid_x, ln_mean, ln_rstd, ln_gain, grad_y, w_qkv, w_out, w_up, w_down):
        tokens, d = resid_x.shape
        hd = w_out.shape[1]
        rot = hd // 4
        positions = jnp.arange(tokens, dtype=F32)[None, :]
        inv_freq = jnp.power(10000.0, -2.0 * jnp.arange(rot // 2, dtype=F32) / rot)
        angles = positions * inv_freq[:, None]
        cos_t, sin_t = jnp.cos(angles), jnp.sin(angles)
        mean, rstd, gain = ln_mean[None, :], ln_rstd[None, :], ln_gain[None, :]
        normed, *qkv, stat = qkv_call(resid_x, mean, rstd, gain, w_qkv, cos_t, sin_t)
        grad_x, gw_up, gw_qkv, gw_down, gw_out = copy_call(layer_call(mesh, qkv, stat, resid_x, normed, grad_y, w_out, w_up, w_down, w_qkv, gain, cos_t, sin_t))
        return grad_x, gw_qkv, gw_out, gw_up, gw_down

    in_specs = (P("data", None), P("data"), P("data"), P(None), P("data", None), P(None, "model"), P("model", None, None), P(None, "model"), P("model", None))
    out_specs = (P("data", None), P("data", "model"), P(("data", "model"), None, None), P("data", "model"), P(("data", "model"), None))
    return jax.shard_map(device_step, mesh=mesh, in_specs=in_specs, out_specs=out_specs, check_vma=False)
```
